128 devices in a mesh: gx: 8 (over y, core), gy: 16 (over x, z).
Axes of the slice: x: 4, y: 4, z: 4, core: 2. Of those that a mesh axis runs over, the one named last changes fastest.
Arguments:
- old_master: float32 [128, 128, 1536], P('gx', 'gy'), may hold values from -3 to 3
- old_first: float32 [128, 128, 1536], P('gx', 'gy'), may hold values from -3 to 3
- old_second: float32 [128, 128, 1536], P('gx', 'gy'), may hold values from 0.01 to 1
- new_grad: bfloat16 [128, 128, 1536], P(('gx', 'gy')), may hold values from -12288 to 12288
- counts: int32 [128, 128], P(None, ('gx', 'gy')), may hold values from 1 to 72, as said below
- old_owner: int32 [128], replicated, may hold values from 0 to 127, each once
- new_owner: int32 [128], replicated, may hold values from 0 to 127, each once
Outputs:
- new_master: float32 [128, 128, 1536], P(('gx', 'gy'))
- new_first: float32 [128, 128, 1536], P(('gx', 'gy'))
- new_second: float32 [128, 128, 1536], P(('gx', 'gy'))
The draws below stay inside these ranges and needn't reach their ends.
Inputs may be any that keep to these rules, and one draw needn't show every extreme that they name: `old_owner`: every number of 0 to 127 appears once. `new_owner`: every number of 0 to 127 appears once. `counts`: every device routed at least one token to every expert.
All inputs are finite; a program needn't handle non-finite values.
Results may differ from the reference program's by a relative error of at most 0.0003.
Values sent between devices are 32-bit elements; how exact they have to be, the bound alone decides.
A program may use at most 64 MiB of HBM per device.

```python
import math
import jax
import jax.numpy as jnp
from jax import lax

FF = 1536
ROWS = 128
EXPERTS = 128
RANKS = 128


def draw_counts(key, part):
    key_tokens = jax.random.fold_in(key, 11)
    key_skew = jax.random.fold_in(key, 23)
    columns = jnp.arange(RANKS, dtype=jnp.int32)
    ceiling = 6 + 12 * columns // max(RANKS - 1, 1)
    factor = 1 + jax.random.randint(key_skew, (EXPERTS,), 0, 4)
    base = 1 + jax.random.randint(key_tokens, (EXPERTS, RANKS), 0, ceiling[None, :])
    return (base * factor[:, None]).astype(jnp.int32)


def block_scale(stream_key, dims, pieces, low, top_value):
    def one(axis_at, parts):
        heights = jax.random.uniform(jax.random.fold_in(jax.random.fold_in(stream_key, 6), axis_at), (parts,), jnp.float32, low / len(pieces), top_value / len(pieces))
        return jnp.repeat(jnp.exp(heights), dims[axis_at] // parts).reshape((-1,) + (1,) * (len(dims) - axis_at - 1))

    level = one(*pieces[0])
    for cut in pieces[1:]:
        level = level * one(*cut)
    return level


def bell_draw(key, extent, scale, limit, cuts=(), kind=jnp.bfloat16):
    values = jax.random.normal(key, extent, jnp.float32) * scale
    if len(cuts) > 0:
        values = block_scale(key, extent, cuts, -0.22, 0.18) * values
    return jnp.clip(values, min=-limit, max=limit).astype(kind)


def setup_inputs(seed: int = 0) -> dict:
    seeds = jax.random.split(jax.random.key(seed), 8)
    old_master = bell_draw(seeds[0], (EXPERTS, ROWS, FF), 0.5, 3.0, ((0, 8), (1, 16)), jnp.float32)
    old_first = bell_draw(seeds[1], (EXPERTS, ROWS, FF), 0.5, 3.0, ((0, 8), (1, 16)), jnp.float32)
    old_second = jnp.clip(jnp.exp(math.log(1.0) - 4.6051702 * jax.random.uniform(seeds[2], (EXPERTS, ROWS, FF), jnp.float32) ** block_scale(seeds[2], (EXPERTS, ROWS, FF), ((0, 8), (1, 16)), -0.2, 0.2)), 0.01, 1.0)
    new_grad = bell_draw(seeds[3], (EXPERTS, ROWS, FF), (16 * EXPERTS), 12288.0, ((0, 128),))
    counts = draw_counts(jax.random.fold_in(seeds[7], 71), 0)
    old_owner = jax.random.permutation(seeds[5], EXPERTS).astype(jnp.int32)
    new_owner = jax.random.permutation(seeds[6], EXPERTS).astype(jnp.int32)
    return {"old_master": old_master, "old_first": old_first, "old_second": old_second, "new_grad": new_grad, "counts": counts, "old_owner": old_owner, "new_owner": new_owner}


first_correction = 1.0 - 0.9 ** 10
second_correction = 1.0 - 0.999 ** 10

def adam_step(master, first, second, grad, slot_count):
    scaled = grad.astype(jnp.float32) / slot_count
    new_first = 0.9 * first + 0.1 * scaled
    new_second = 0.999 * second + 0.001 * scaled * scaled
    step_dir = new_first / first_correction / (jnp.sqrt(new_second / second_correction) + 1e-08)
    new_master = master - 0.01 * (step_dir + 0.1 * master)
    return (new_master, new_first, new_second)

def reference(old_master, old_first, old_second, new_grad, counts, old_owner, new_owner):
    slots = jnp.arange(EXPERTS, dtype=jnp.int32)
    onehot = new_owner[:, None] == slots[None, :]
    source = lax.optimization_barrier(jnp.sum(jnp.where(onehot, old_owner[:, None], 0), axis=0)).astype(jnp.int32)
    totals = lax.optimization_barrier(jnp.sum(counts.astype(jnp.float32), axis=1))
    slot_count = lax.optimization_barrier(jnp.sum(jnp.where(onehot, totals[:, None], jnp.float32(0.0)), axis=0))
    master = jnp.take(old_master, source, axis=0)
    first = jnp.take(old_first, source, axis=0)
    second = jnp.take(old_second, source, axis=0)
    return adam_step(master, first, second, new_grad, slot_count[:, None, None])
```

```python
import functools

import jax
import jax.numpy as jnp
from jax import lax
from jax.experimental import pallas as pl
from jax.experimental.pallas import tpu as pltpu
from jax.sharding import PartitionSpec as P

MESH = pl.DeviceIdType.MESH
LANES = 128
ORDER = (1, 3, 2)
Z_LAG = 2
Y_LAG = 4

first_correction = 1.0 - 0.9**10
second_correction = 1.0 - 0.999**10


def device(x, y, z, c):
    return (y * 2 + c, x * 4 + z)


def mod4(v):
    return lax.rem(v + 4, 4)


def exchange_kernel(
    chunks, third, source_ref, counts_ref, *refs
):
    states, (outs, totals_ref), scratch = refs[:3], (refs[3:6], refs[6]), refs[7:]
    n = len(chunks)
    a_bufs, b_bufs, c_bufs, d_bufs = (scratch[i * n : (i + 1) * n] for i in range(4))
    count_g, count_x, count_z, sx, sz = scratch[4 * n : 4 * n + 5]
    sems = scratch[4 * n + 5 :]
    y1_send, y1_recv, own_sem, core_send, core_recv, x_send, x_recv = sems[:7]
    z_send, z_recv, y2_send, y2_recv, out_sem, n_send, n_recv = sems[7:]

    gx, gy = lax.axis_index("gx"), lax.axis_index("gy")
    x, y, z, c = lax.div(gy, 4), lax.div(gx, 2), lax.rem(gy, 4), lax.rem(gx, 2)
    other = 1 - c

    xs = [device(mod4(x + d), y, z, c) for d in range(4)]
    ys = [device(x, mod4(y + d), z, c) for d in range(4)]
    zs = [device(x, y, mod4(z + d), c) for d in range(4)]
    gs = [(lax.rem(gx + d, 8), gy) for d in range(8)]

    barrier = pltpu.get_barrier_semaphore()
    for peer in gs[1:] + xs[1:] + zs[1:]:
        pl.semaphore_signal(barrier, inc=1, device_id=peer, device_id_type=MESH)
    pl.semaphore_wait(barrier, 13)

    started = []

    def remote(src, dst, send, recv, peer):
        copy = pltpu.make_async_remote_copy(
            src_ref=src, dst_ref=dst, send_sem=send, recv_sem=recv, device_id=peer, device_id_type=MESH
        )
        copy.start()
        started.append(copy)
        return copy

    def block(owner_y, owner_c):
        return pl.ds(pl.multiple_of((owner_y * 2 + owner_c) * 16, 16), 16)

    def columns(owner_y, offset, width):
        return pl.ds(pl.multiple_of(owner_y * third + offset, LANES), width)

    count_g[pl.ds(gx, 1)] = counts_ref[...].reshape(1, 1, LANES)
    y1, own, cores = [], [], []
    for k, (s, offset, width) in enumerate(chunks):
        y1.append(
            {
                d: remote(
                    states[s].at[:, :, columns(mod4(y + d), offset, width)],
                    a_bufs[k].at[block(y, c)],
                    y1_send.at[k, d],
                    y1_recv.at[k, d],
                    ys[d],
                )
                for d in ORDER
            }
        )
        mine = states[s].at[:, :, columns(y, offset, width)]
        local = pltpu.make_async_copy(mine, a_bufs[k].at[block(y, c)], own_sem.at[k])
        local.start()
        own.append(local)
        cores.append(
            {0: remote(mine, a_bufs[k].at[block(y, c)], core_send.at[k, 0], core_recv.at[k, 0], gs_partner(x, y, z, other))}
        )
        if k == 0:
            tallies = [
                remote(counts_ref, count_g.at[gx], n_send.at[d], n_recv.at[d], gs[d]) for d in range(1, 8)
            ]

    def forward(k):
        for d in ORDER:
            y1[k][d].wait_recv()
            held = a_bufs[k].at[block(mod4(y - d), c)]
            cores[k][d] = remote(held, held, core_send.at[k, d], core_recv.at[k, d], gs_partner(x, y, z, other))

    sent_x, sent_z, sent_y = {}, {}, {}

    def permute(k):
        own[k].wait()
        for d in range(4):
            cores[k][d].wait_recv()
        for d in range(4):
            base = 4 * mod4(x + d) + 16 * c

            def place(j, carry, d=d, base=base):
                to_z, to_y = lax.div(j, 4), lax.rem(j, 4)
                tile = a_bufs[k][source_ref[base + 32 * to_y + to_z]]
                if d == 0:
                    c_bufs[k][x, to_z, to_y] = tile
                else:
                    b_bufs[k][d - 1, to_z, to_y] = tile
                return carry

            lax.fori_loop(0, 16, place, 0, unroll=4)
        sent_x[k] = [
            remote(b_bufs[k].at[d - 1], c_bufs[k].at[x], x_send.at[k, d], x_recv.at[k, d], xs[d]) for d in ORDER
        ]

    def along_z(k):
        for copy in sent_x[k]:
            copy.wait_recv()
        sent_z[k] = [
            remote(
                c_bufs[k].at[:, mod4(z + d)], d_bufs[k].at[:, z], z_send.at[k, d], z_recv.at[k, d], zs[d]
            )
            for d in ORDER
        ]
        d_bufs[k][:, pl.ds(z, 1)] = c_bufs[k][:, pl.ds(z, 1)]

    def along_y(k):
        s, offset, width = chunks[k]
        for copy in sent_z[k]:
            copy.wait_recv()
        landing = outs[s].at[:, :, :, columns(y, offset, width)]
        sent_y[k] = [
            remote(d_bufs[k].at[:, :, mod4(y + d)], landing, y2_send.at[k, d], y2_recv.at[k, d], ys[d])
            for d in ORDER
        ]
        local = pltpu.make_async_copy(d_bufs[k].at[:, :, y], landing, out_sem.at[k])
        local.start()
        own[k] = local

    def tally_x():
        for copy in tallies:
            copy.wait_recv()
        count = jnp.sum(count_g[...], axis=0)
        sx[...] = count
        count_x[pl.ds(x, 1)] = count.reshape(1, 1, LANES)

    def tally_send_x():
        return [
            remote(sx, count_x.at[x], n_send.at[7 + d], n_recv.at[7 + d], xs[d]) for d in range(1, 4)
        ]

    def tally_z(copies):
        for copy in copies:
            copy.wait_recv()
        count = jnp.sum(count_x[...], axis=0)
        sz[...] = count
        count_z[pl.ds(z, 1)] = count.reshape(1, 1, LANES)

    def tally_send_z():
        return [
            remote(sz, count_z.at[z], n_send.at[10 + d], n_recv.at[10 + d], zs[d]) for d in range(1, 4)
        ]

    counted = None
    for i in range(n + Y_LAG):
        if i < n:
            forward(i)
        if 0 <= i - Y_LAG < n:
            along_y(i - Y_LAG)
        if 0 <= i - Z_LAG < n:
            along_z(i - Z_LAG)
        if i == 1:
            counted = tally_send_x()
        if i == 4:
            counted = tally_send_z()
        if i < n:
            permute(i)
        if i == 0:
            tally_x()
        if i == 3:
            tally_z(counted)
    for copy in counted:
        copy.wait_recv()
    totals_ref[...] = jnp.sum(count_z[...], axis=0)
    for k in range(n):
        own[k].wait()
        for copy in sent_y[k]:
            copy.wait_recv()
    for copy in started:
        copy.wait_send()


def gs_partner(x, y, z, other):
    return device(x, y, z, other)


def adam_step(master, first, second, grad, slot_count):
    scaled = grad.astype(jnp.float32) / slot_count
    new_first = 0.9 * first + 0.1 * scaled
    new_second = 0.999 * second + 0.001 * scaled * scaled
    step_dir = new_first / first_correction / (jnp.sqrt(new_second / second_correction) + 1e-08)
    new_master = master - 0.01 * (step_dir + 0.1 * master)
    return (new_master, new_first, new_second)


def body(old_master, old_first, old_second, new_grad, counts, old_owner, new_owner):
    experts = old_owner.shape[0]
    group, rows, ff = old_master.shape
    third = ff // 4
    my_slot = lax.axis_index("gx") * lax.axis_size("gy") + lax.axis_index("gy")
    slots = jnp.arange(experts, dtype=jnp.int32)
    onehot = new_owner[:, None] == slots[None, :]
    source = jnp.sum(jnp.where(onehot, old_owner[:, None], 0), axis=0)
    local_counts = counts.astype(jnp.float32).reshape(1, experts)

    chunks = [(s, offset, LANES) for s in range(3) for offset in range(0, third, LANES)]
    n = len(chunks)
    f32 = jnp.float32
    dma = pltpu.SemaphoreType.DMA
    scratch = (
        [pltpu.VMEM((experts, rows, w), f32) for _, _, w in chunks]
        + [pltpu.VMEM((3, 4, 4, rows, w), f32) for _, _, w in chunks]
        + [pltpu.VMEM((4, 4, 4, rows, w), f32) for _, _, w in chunks]
        + [pltpu.VMEM((4, 4, 4, rows, w), f32) for _, _, w in chunks]
        + [pltpu.VMEM((8, 1, experts), f32), pltpu.VMEM((4, 1, experts), f32), pltpu.VMEM((4, 1, experts), f32)]
        + [pltpu.VMEM((1, experts), f32), pltpu.VMEM((1, experts), f32)]
        + [dma((n, 4)), dma((n, 4)), dma((n,)), dma((n, 4)), dma((n, 4)), dma((n, 4)), dma((n, 4))]
        + [dma((n, 4)), dma((n, 4)), dma((n, 4)), dma((n, 4)), dma((n,)), dma((14,)), dma((14,))]
    )
    landed = jax.ShapeDtypeStruct((4, 4, rows, ff), f32)
    vmem, hbm = pl.BlockSpec(memory_space=pltpu.VMEM), pl.BlockSpec(memory_space=pl.ANY)
    master, first, second, totals = pl.pallas_call(
        functools.partial(exchange_kernel, chunks, third),
        name="exchange",
        out_shape=(landed, landed, landed, jax.ShapeDtypeStruct((1, experts), f32)),
        in_specs=[pl.BlockSpec(memory_space=pltpu.SMEM), vmem, hbm, hbm, hbm],
        out_specs=(hbm, hbm, hbm, vmem),
        scratch_shapes=scratch,
        compiler_params=pltpu.CompilerParams(
            collective_id=0, has_side_effects=True, vmem_limit_bytes=60 * 1024 * 1024
        ),
    )(source, local_counts, old_master, old_first, old_second)
    shape = (1, 16 * rows, ff)
    slot_count = jnp.sum(jnp.where(new_owner == my_slot, totals[0], jnp.float32(0.0)))
    return adam_step(master.reshape(shape), first.reshape(shape), second.reshape(shape), new_grad, slot_count)


def solution(mesh):
    placed = (
        P("gx", "gy", None),
        P("gx", "gy", None),
        P("gx", "gy", None),
        P(("gx", "gy"), None, None),
        P(None, ("gx", "gy")),
        P(),
        P(),
    )
    out = P(("gx", "gy"), None, None)
    return jax.shard_map(body, mesh=mesh, in_specs=placed, out_specs=(out, out, out), check_vma=False)
```

```python
import functools

import jax
import jax.numpy as jnp
from jax import lax
from jax.experimental import pallas as pl
from jax.experimental.pallas import tpu as pltpu
from jax.sharding import PartitionSpec as P

MESH = pl.DeviceIdType.MESH
LANES = 128
ORDER = (1, 3, 2)
Z_LAG = 2
Y_LAG = 4
ADAM_ROWS = 32

first_correction = 1.0 - 0.9**10
second_correction = 1.0 - 0.999**10


def device(x, y, z, c):
    return (y * 2 + c, x * 4 + z)


def mod4(v):
    return lax.rem(v + 4, 4)


def exchange_kernel(
    chunks, quarter, counts_ref, old_owner_ref, new_owner_ref, *refs
):
    states, (outs, slot_count_ref), scratch = refs[:3], (refs[3:6], refs[6]), refs[7:]
    n = len(chunks)
    a_bufs, b_bufs, c_bufs, d_bufs = (scratch[i * n : (i + 1) * n] for i in range(4))
    count_g, count_x, count_z, sx, sz, owners, source_row, source_ref = scratch[4 * n : 4 * n + 8]
    sems = scratch[4 * n + 8 :]
    y1_send, y1_recv, own_sem, core_send, core_recv, x_send, x_recv = sems[:7]
    z_send, z_recv, y2_send, y2_recv, out_sem, n_send, n_recv, small_sem = sems[7:]

    gx, gy = lax.axis_index("gx"), lax.axis_index("gy")
    x, y, z, c = lax.div(gy, 4), lax.div(gx, 2), lax.rem(gy, 4), lax.rem(gx, 2)
    other = 1 - c

    xs = [device(mod4(x + d), y, z, c) for d in range(4)]
    ys = [device(x, mod4(y + d), z, c) for d in range(4)]
    zs = [device(x, y, mod4(z + d), c) for d in range(4)]
    gs = [(lax.rem(gx + d, 8), gy) for d in range(8)]

    barrier = pltpu.get_barrier_semaphore()
    for peer in gs[1:] + xs[1:] + zs[1:]:
        pl.semaphore_signal(barrier, inc=1, device_id=peer, device_id_type=MESH)
    pl.semaphore_wait(barrier, 13)

    started = []

    def remote(src, dst, send, recv, peer):
        copy = pltpu.make_async_remote_copy(
            src_ref=src, dst_ref=dst, send_sem=send, recv_sem=recv, device_id=peer, device_id_type=MESH
        )
        copy.start()
        started.append(copy)
        return copy

    def block(owner_y, owner_c):
        return pl.ds(pl.multiple_of((owner_y * 2 + owner_c) * 16, 16), 16)

    def columns(owner_y, offset, width):
        return pl.ds(pl.multiple_of(owner_y * quarter + offset, LANES), width)

    small = [
        pltpu.make_async_copy(old_owner_ref, owners.at[0], small_sem.at[0]),
        pltpu.make_async_copy(new_owner_ref, owners.at[1], small_sem.at[1]),
        pltpu.make_async_copy(counts_ref, count_g.at[gx], small_sem.at[2]),
    ]
    for copy in small:
        copy.start()
    y1, own, cores = [], [], []
    for k, (s, offset, width) in enumerate(chunks):
        y1.append(
            {
                d: remote(
                    states[s].at[:, :, columns(mod4(y + d), offset, width)],
                    a_bufs[k].at[block(y, c)],
                    y1_send.at[k, d],
                    y1_recv.at[k, d],
                    ys[d],
                )
                for d in ORDER
            }
        )
        mine = states[s].at[:, :, columns(y, offset, width)]
        local = pltpu.make_async_copy(mine, a_bufs[k].at[block(y, c)], own_sem.at[k])
        local.start()
        own.append(local)
        cores.append(
            {0: remote(mine, a_bufs[k].at[block(y, c)], core_send.at[k, 0], core_recv.at[k, 0], gs_partner(x, y, z, other))}
        )
        if k == 0:
            tallies = [
                remote(counts_ref, count_g.at[gx], n_send.at[d], n_recv.at[d], gs[d]) for d in range(1, 8)
            ]

    for copy in small:
        copy.wait()
    old_column = jnp.broadcast_to(owners[0], (LANES, LANES)).T
    new_column = jnp.broadcast_to(owners[1], (LANES, LANES)).T
    lanes = lax.broadcasted_iota(jnp.int32, (LANES, LANES), 1)
    source_row[...] = jnp.sum(jnp.where(new_column == lanes, old_column, 0), axis=0, keepdims=True)
    to_scalar = pltpu.make_async_copy(source_row, source_ref, small_sem.at[3])
    to_scalar.start()

    def forward(k):
        for d in ORDER:
            y1[k][d].wait_recv()
            held = a_bufs[k].at[block(mod4(y - d), c)]
            cores[k][d] = remote(held, held, core_send.at[k, d], core_recv.at[k, d], gs_partner(x, y, z, other))

    sent_x, sent_z, sent_y = {}, {}, {}

    def permute(k):
        own[k].wait()
        for d in range(4):
            cores[k][d].wait_recv()
        for d in range(4):
            base = 4 * mod4(x + d) + 16 * c

            def place(j, carry, d=d, base=base):
                to_z, to_y = lax.div(j, 4), lax.rem(j, 4)
                tile = a_bufs[k][source_ref[0, base + 32 * to_y + to_z]]
                if d == 0:
                    c_bufs[k][x, to_z, to_y] = tile
                else:
                    b_bufs[k][d - 1, to_z, to_y] = tile
                return carry

            lax.fori_loop(0, 16, place, 0, unroll=4)
        sent_x[k] = [
            remote(b_bufs[k].at[d - 1], c_bufs[k].at[x], x_send.at[k, d], x_recv.at[k, d], xs[d]) for d in ORDER
        ]

    def along_z(k):
        for copy in sent_x[k]:
            copy.wait_recv()
        sent_z[k] = [
            remote(
                c_bufs[k].at[:, mod4(z + d)], d_bufs[k].at[:, z], z_send.at[k, d], z_recv.at[k, d], zs[d]
            )
            for d in ORDER
        ]
        d_bufs[k][:, pl.ds(z, 1)] = c_bufs[k][:, pl.ds(z, 1)]

    def along_y(k):
        s, offset, width = chunks[k]
        for copy in sent_z[k]:
            copy.wait_recv()
        landing = outs[s].at[:, :, :, columns(y, offset, width)]
        sent_y[k] = [
            remote(d_bufs[k].at[:, :, mod4(y + d)], landing, y2_send.at[k, d], y2_recv.at[k, d], ys[d])
            for d in ORDER
        ]
        local = pltpu.make_async_copy(d_bufs[k].at[:, :, y], landing, out_sem.at[k])
        local.start()
        own[k] = local

    def tally_x():
        for copy in tallies:
            copy.wait_recv()
        count = jnp.sum(count_g[...].astype(jnp.float32), axis=0)
        sx[...] = count
        count_x[pl.ds(x, 1)] = count.reshape(1, 1, LANES)

    def tally_send_x():
        return [
            remote(sx, count_x.at[x], n_send.at[7 + d], n_recv.at[7 + d], xs[d]) for d in range(1, 4)
        ]

    def tally_z(copies):
        for copy in copies:
            copy.wait_recv()
        count = jnp.sum(count_x[...], axis=0)
        sz[...] = count
        count_z[pl.ds(z, 1)] = count.reshape(1, 1, LANES)

    def tally_send_z():
        return [
            remote(sz, count_z.at[z], n_send.at[10 + d], n_recv.at[10 + d], zs[d]) for d in range(1, 4)
        ]

    counted = None
    for i in range(n + Y_LAG):
        if i < n:
            forward(i)
        if 0 <= i - Y_LAG < n:
            along_y(i - Y_LAG)
        if 0 <= i - Z_LAG < n:
            along_z(i - Z_LAG)
        if i == 1:
            counted = tally_send_x()
        if i == 4:
            counted = tally_send_z()
        if i == 0:
            to_scalar.wait()
        if i < n:
            permute(i)
        if i == 0:
            tally_x()
        if i == 3:
            tally_z(counted)
    for copy in counted:
        copy.wait_recv()
    totals = jnp.sum(count_z[...], axis=0)
    mine = jnp.where(owners[1] == gx * 16 + gy, totals, 0.0)
    slot_count_ref[...] = jnp.broadcast_to(jnp.sum(mine, axis=1, keepdims=True), (1, LANES))
    for k in range(n):
        own[k].wait()
        for copy in sent_y[k]:
            copy.wait_recv()
    for copy in started:
        copy.wait_send()


def gs_partner(x, y, z, other):
    return device(x, y, z, other)


def adam_kernel(slot_count, master, first, second, grad, new_master, new_first, new_second):
    scaled = grad[0].astype(jnp.float32) / slot_count[0:1, 0:1]
    moved_first = 0.9 * first[0] + 0.1 * scaled
    moved_second = 0.999 * second[0] + 0.001 * scaled * scaled
    step_dir = moved_first / first_correction / (jnp.sqrt(moved_second / second_correction) + 1e-08)
    new_master[0] = master[0] - 0.01 * (step_dir + 0.1 * master[0])
    new_first[0] = moved_first
    new_second[0] = moved_second


def adam_step(master, first, second, grad, slot_count, block_rows=ADAM_ROWS):
    _, rows, ff = grad.shape
    tile = pl.BlockSpec((1, block_rows, ff), lambda i: (0, i, 0))
    state = jax.ShapeDtypeStruct((1, rows, ff), jnp.float32)
    return pl.pallas_call(
        adam_kernel,
        name="adam",
        grid=(rows // block_rows,),
        out_shape=(state, state, state),
        in_specs=[pl.BlockSpec((1, LANES), lambda i: (0, 0)), tile, tile, tile, tile],
        out_specs=(tile, tile, tile),
    )(slot_count, master, first, second, grad)


def body(old_master, old_first, old_second, new_grad, counts, old_owner, new_owner):
    experts = old_owner.shape[0]
    group, rows, ff = old_master.shape
    quarter = ff // 4
    row = (1, experts)

    chunks = [(s, offset, LANES) for s in range(3) for offset in range(0, quarter, LANES)]
    n = len(chunks)
    f32 = jnp.float32
    dma = pltpu.SemaphoreType.DMA
    scratch = (
        [pltpu.VMEM((experts, rows, w), f32) for _, _, w in chunks]
        + [pltpu.VMEM((3, 4, 4, rows, w), f32) for _, _, w in chunks]
        + [pltpu.VMEM((4, 4, 4, rows, w), f32) for _, _, w in chunks]
        + [pltpu.VMEM((4, 4, 4, rows, w), f32) for _, _, w in chunks]
        + [pltpu.VMEM((8, 1, experts), jnp.int32), pltpu.VMEM((4, 1, experts), f32), pltpu.VMEM((4, 1, experts), f32)]
        + [pltpu.VMEM((1, experts), f32), pltpu.VMEM((1, experts), f32), pltpu.VMEM((2, 1, experts), jnp.int32)]
        + [pltpu.VMEM((1, experts), jnp.int32), pltpu.SMEM((1, experts), jnp.int32)]
        + [dma((n, 4)), dma((n, 4)), dma((n,)), dma((n, 4)), dma((n, 4)), dma((n, 4)), dma((n, 4))]
        + [dma((n, 4)), dma((n, 4)), dma((n, 4)), dma((n, 4)), dma((n,)), dma((14,)), dma((14,)), dma((4,))]
    )
    landed = jax.ShapeDtypeStruct((4, 4, rows, ff), f32)
    vmem, hbm = pl.BlockSpec(memory_space=pltpu.VMEM), pl.BlockSpec(memory_space=pl.ANY)
    master, first, second, slot_count = pl.pallas_call(
        functools.partial(exchange_kernel, chunks, quarter),
        name="exchange",
        out_shape=(landed, landed, landed, jax.ShapeDtypeStruct((1, experts), f32)),
        in_specs=[hbm] * 6,
        out_specs=(hbm, hbm, hbm, vmem),
        scratch_shapes=scratch,
        compiler_params=pltpu.CompilerParams(
            collective_id=0, has_side_effects=True, vmem_limit_bytes=60 * 1024 * 1024
        ),
    )(counts.reshape(row), old_owner.reshape(row), new_owner.reshape(row), old_master, old_first, old_second)
    shape = (1, 16 * rows, ff)
    return adam_step(master.reshape(shape), first.reshape(shape), second.reshape(shape), new_grad, slot_count)


def solution(mesh):
    placed = (
        P("gx", "gy", None),
        P("gx", "gy", None),
        P("gx", "gy", None),
        P(("gx", "gy"), None, None),
        P(None, ("gx", "gy")),
        P(),
        P(),
    )
    out = P(("gx", "gy"), None, None)
    return jax.shard_map(body, mesh=mesh, in_specs=placed, out_specs=(out, out, out), check_vma=False)
```

```python
import functools

import jax
import jax.numpy as jnp
from jax import lax
from jax.experimental import pallas as pl
from jax.experimental.pallas import tpu as pltpu
from jax.sharding import PartitionSpec as P

MESH = pl.DeviceIdType.MESH
LANES = 128
ORDER = (1, 3, 2)
Z_LAG = 2
Y_LAG = 4
ADAM_ROWS = 32
DEPTH = 2
TIERS = ((9, 9), (10, 10))
WIDTHS = ((2, 2, 2), (2, 2, 2), (2, 2, 1, 1))

first_correction = 1.0 - 0.9**10
second_correction = 1.0 - 0.999**10


def device(x, y, z, c):
    return (y * 2 + c, x * 4 + z)


def mod4(v):
    return lax.rem(v + 4, 4)


def exchange_kernel(
    chunks, quarter, table_ref, counts_ref, old_owner_ref, new_owner_ref, *refs
):
    states, (outs, slot_count_ref), scratch = refs[:3], (refs[3:6], refs[6]), refs[7:]
    n = len(chunks)
    a_bufs, b_bufs, c_bufs, d_bufs = (scratch[i * n : (i + 1) * n] for i in range(4))
    count_g, count_x, count_z, sx, sz, owners, source_row, source_ref = scratch[4 * n : 4 * n + 8]
    sems = scratch[4 * n + 8 :]
    y1_send, y1_recv, own_sem, core_send, core_recv, x_send, x_recv = sems[:7]
    z_send, z_recv, y2_send, y2_recv, out_sem, n_send, n_recv, small_sem = sems[7:]

    gx, gy = lax.axis_index("gx"), lax.axis_index("gy")
    x, y, z, c = lax.div(gy, 4), lax.div(gx, 2), lax.rem(gy, 4), lax.rem(gx, 2)
    other = 1 - c

    xs = [device(mod4(x + d), y, z, c) for d in range(4)]
    ys = [device(x, mod4(y + d), z, c) for d in range(4)]
    zs = [device(x, y, mod4(z + d), c) for d in range(4)]
    gs = [(lax.rem(gx + d, 8), gy) for d in range(8)]

    barrier = pltpu.get_barrier_semaphore()
    for peer in gs[1:] + xs[1:] + zs[1:]:
        pl.semaphore_signal(barrier, inc=1, device_id=peer, device_id_type=MESH)
    pl.semaphore_wait(barrier, 13)

    started = []

    def remote(src, dst, send, recv, peer):
        copy = pltpu.make_async_remote_copy(
            src_ref=src, dst_ref=dst, send_sem=send, recv_sem=recv, device_id=peer, device_id_type=MESH
        )
        copy.start()
        started.append(copy)
        return copy

    def block(owner_y, owner_c):
        return pl.ds(pl.multiple_of((owner_y * 2 + owner_c) * 16, 16), 16)

    def columns(owner_y, offset, width):
        return pl.ds(pl.multiple_of(owner_y * quarter + offset, LANES), width)

    small = [
        pltpu.make_async_copy(old_owner_ref, owners.at[0], small_sem.at[0]),
        pltpu.make_async_copy(new_owner_ref, owners.at[1], small_sem.at[1]),
        pltpu.make_async_copy(counts_ref, count_g.at[gx], small_sem.at[2]),
    ]
    for copy in small:
        copy.start()
    y1, own, cores = [], [], []
    for k, (s, offset, width) in enumerate(chunks):
        y1.append(
            {
                d: remote(
                    states[s].at[:, :, columns(mod4(y + d), offset, width)],
                    a_bufs[k].at[block(y, c)],
                    y1_send.at[k, d],
                    y1_recv.at[k, d],
                    ys[d],
                )
                for d in ORDER
            }
        )
        mine = states[s].at[:, :, columns(y, offset, width)]
        local = pltpu.make_async_copy(mine, a_bufs[k].at[block(y, c)], own_sem.at[k])
        local.start()
        own.append(local)
        cores.append(
            {0: remote(mine, a_bufs[k].at[block(y, c)], core_send.at[k, 0], core_recv.at[k, 0], gs_partner(x, y, z, other))}
        )
        if k == 0:
            tallies = [
                remote(counts_ref, count_g.at[gx], n_send.at[d], n_recv.at[d], gs[d]) for d in range(1, 8)
            ]

    for copy in small:
        copy.wait()
    old_column = jnp.broadcast_to(owners[0], (LANES, LANES)).T
    new_column = jnp.broadcast_to(owners[1], (LANES, LANES)).T
    lanes = lax.broadcasted_iota(jnp.int32, (LANES, LANES), 1)
    source_row[...] = jnp.sum(jnp.where(new_column == lanes, old_column, 0), axis=0, keepdims=True)
    to_scalar = pltpu.make_async_copy(source_row, source_ref, small_sem.at[3])
    to_scalar.start()

    def forward(k):
        for d in ORDER:
            y1[k][d].wait_recv()
            held = a_bufs[k].at[block(mod4(y - d), c)]
            cores[k][d] = remote(held, held, core_send.at[k, d], core_recv.at[k, d], gs_partner(x, y, z, other))

    sent_x, sent_z, sent_y = {}, {}, {}

    def permute(k):
        own[k].wait()
        for d in range(4):
            cores[k][d].wait_recv()
        for d in range(4):
            base = 4 * mod4(x + d) + 16 * c

            def place(j, carry, d=d, base=base):
                to_z, to_y = lax.div(j, 4), lax.rem(j, 4)
                tile = a_bufs[k][source_ref[0, base + 32 * to_y + to_z]]
                if d == 0:
                    c_bufs[k][x, to_z, to_y] = tile
                else:
                    b_bufs[k][d - 1, to_z, to_y] = tile
                return carry

            lax.fori_loop(0, 16, place, 0, unroll=4)
        sent_x[k] = [
            remote(b_bufs[k].at[d - 1], c_bufs[k].at[x], x_send.at[k, d], x_recv.at[k, d], xs[d]) for d in ORDER
        ]

    def along_z(k):
        for copy in sent_x[k]:
            copy.wait_recv()
        sent_z[k] = [
            remote(
                c_bufs[k].at[:, mod4(z + d)], d_bufs[k].at[:, z], z_send.at[k, d], z_recv.at[k, d], zs[d]
            )
            for d in ORDER
        ]
        d_bufs[k][:, pl.ds(z, 1)] = c_bufs[k][:, pl.ds(z, 1)]

    def along_y(k):
        s, offset, width = chunks[k]
        for copy in sent_z[k]:
            copy.wait_recv()
        landing = outs[s].at[:, :, :, columns(y, offset, width)]
        sent_y[k] = [
            remote(d_bufs[k].at[:, :, mod4(y + d)], landing, y2_send.at[k, d], y2_recv.at[k, d], ys[d])
            for d in ORDER
        ]
        local = pltpu.make_async_copy(d_bufs[k].at[:, :, y], landing, out_sem.at[k])
        local.start()
        own[k] = local

    def tally_x():
        for copy in tallies:
            copy.wait_recv()
        count = jnp.sum(count_g[...].astype(jnp.float32), axis=0)
        sx[...] = count
        count_x[pl.ds(x, 1)] = count.reshape(1, 1, LANES)

    def tally_send_x():
        return [
            remote(sx, count_x.at[x], n_send.at[7 + d], n_recv.at[7 + d], xs[d]) for d in range(1, 4)
        ]

    def tally_z(copies):
        for copy in copies:
            copy.wait_recv()
        count = jnp.sum(count_x[...], axis=0)
        sz[...] = count
        count_z[pl.ds(z, 1)] = count.reshape(1, 1, LANES)

    def tally_send_z():
        return [
            remote(sz, count_z.at[z], n_send.at[10 + d], n_recv.at[10 + d], zs[d]) for d in range(1, 4)
        ]

    counted = None
    for i in range(n + Y_LAG):
        if i < n:
            forward(i)
        if 0 <= i - Y_LAG < n:
            along_y(i - Y_LAG)
        if 0 <= i - Z_LAG < n:
            along_z(i - Z_LAG)
        if i == 1:
            counted = tally_send_x()
        if i == 4:
            counted = tally_send_z()
        if i == 0:
            to_scalar.wait()
        if i < n:
            permute(i)
        if i == 0:
            tally_x()
        if i == 3:
            tally_z(counted)
    for copy in counted:
        copy.wait_recv()
    totals = jnp.sum(count_z[...], axis=0)
    mine = jnp.where(owners[1] == gx * 16 + gy, totals, 0.0)
    slot_count_ref[...] = jnp.broadcast_to(jnp.sum(mine, axis=1, keepdims=True), (1, LANES))
    for k in range(n):
        own[k].wait()
        for copy in sent_y[k]:
            copy.wait_recv()
    for copy in started:
        copy.wait_send()


def gs_partner(x, y, z, other):
    return device(x, y, z, other)


def plan_kernel(old_owner_ref, new_owner_ref, table_ref):
    f32, i32 = jnp.float32, jnp.int32
    square, row = (LANES, LANES), (8, LANES)
    old, new = (jnp.broadcast_to(ref[...], square) for ref in (old_owner_ref, new_owner_ref))
    sub, lane = lax.broadcasted_iota(i32, square, 0), lax.broadcasted_iota(i32, square, 1)

    dest_down = jnp.sum(jnp.where(old == sub, new, 0).astype(f32), axis=1, keepdims=True)
    dest_down = jnp.broadcast_to(dest_down, square)
    dest_across = dest_down.T.astype(i32)
    dest_down = dest_down.astype(i32)
    shift_down = ((dest_down >> 5) - (sub >> 5)) & 3
    shift_across = ((dest_across >> 5) - (lane >> 5)) & 3
    together = (sub >> 5) == (lane >> 5)

    def tally(mask):
        return jnp.broadcast_to(jnp.sum(jnp.where(mask, 1, 0), axis=0, keepdims=True), row)

    rank = tally(together & (shift_down == shift_across) & (sub < lane))
    n1, n2, n3 = (tally(together & (shift_down == d)) for d in (1, 2, 3))

    lane = lane[:8]
    slot, shift, home, own = dest_across[:8], shift_across[:8], lane >> 5, lane & 31

    def before(v):
        return pltpu.roll(v, 32, 1)

    def after(v):
        return pltpu.roll(v, LANES - 32, 1)

    def loads(up):
        down = n2 - up
        return n1 + up + before(up), n3 + down + after(down)

    up = (n2 + (home & 1)) >> 1
    for parity in (0, 1):
        plus, minus = loads(up)
        gap = jnp.maximum(minus, before(minus)) - jnp.maximum(plus, after(plus))
        step = jnp.where(gap < 0, -((-gap) >> 1), gap >> 1)
        up = jnp.where((home & 1) == parity, jnp.clip(up + step, 0, n2), up)
    down = n2 - up
    plus, minus = loads(up)

    def highest(v):
        return jnp.broadcast_to(jnp.max(v.astype(f32), axis=1, keepdims=True), row).astype(i32)

    need, need_far = highest(jnp.maximum(plus, minus)), highest(jnp.maximum(up, down))
    tier = jnp.full(row, len(TIERS), i32)
    first, second = jnp.full(row, TIERS[-1][0], i32), jnp.full(row, TIERS[-1][1], i32)
    for number, (l1, l2) in reversed(list(enumerate(TIERS))):
        fits = (need <= l1 + l2) & (need_far <= min(l1, l2))
        tier = jnp.where(fits, number, tier)
        first, second = jnp.where(fits, l1, first), jnp.where(fits, l2, second)

    here = lax.div(lax.axis_index("gx"), 2)
    mine, from_before, from_after = (
        home == here,
        home == lax.rem(here + 3, 4),
        home == lax.rem(here + 1, 4),
    )
    goes_up = rank < up
    at_up, at_down = up + rank, down + rank
    late_up, late_down = before(up) + at_up - first, after(down) + at_down - first
    one, two, three = shift == 1, shift == 2, shift == 3

    def pick(*cases):
        value = jnp.full(row, -1, i32)
        for mask, case in cases:
            value = jnp.where(mask, case, value)
        return value

    sends = (
        (pick((mine & two & goes_up, rank), (mine & one & (at_up < first), at_up)), own),
        (pick((mine & two & ~goes_up, rank - up), (mine & three & (at_down < first), at_down)), own),
        (
            pick((mine & one & (at_up >= first), late_up), (from_before & two & goes_up, rank)),
            pick((mine, own), (from_before, 32 + rank)),
        ),
        (
            pick((mine & three & (at_down >= first), late_down), (from_after & two & ~goes_up, rank - up)),
            pick((mine, own), (from_after, 32 + first + rank - up)),
        ),
        (
            pick(((slot >> 5) == here, slot & 31)),
            pick(
                (shift == 0, own),
                (one & (at_up < first), 32 + at_up),
                (one & (at_up >= first), 32 + 2 * first + late_up),
                (three & (at_down < first), 32 + first + at_down),
                (three & (at_down >= first), 32 + 2 * first + second + late_down),
                (two & goes_up, 32 + 2 * first + rank),
                (two & ~goes_up, 32 + 2 * first + second + rank - up),
            ),
        ),
    )
    places = lax.broadcasted_iota(i32, (32, LANES), 0)
    lanes = lax.broadcasted_iota(i32, (32, LANES), 1)
    table = jnp.where(lanes == 5, tier[:1], 0).astype(f32)
    for k, (position, value) in enumerate(sends):
        hit = jnp.broadcast_to(position[:1], (32, LANES)) == places
        entry = jnp.sum(jnp.where(hit, value[:1], 0).astype(f32), axis=1, keepdims=True)
        table = jnp.where(lanes == k, entry, table)
    table = jnp.concatenate([table, jnp.zeros((LANES - 32, LANES), f32)], axis=0)
    table_ref[...] = table.T[:8].astype(i32)


def routed_kernel(chunks, half, l1, l2, table_ref, counts_ref, old_owner_ref, new_owner_ref, *refs):
    states, (outs, slot_count_ref), scratch = refs[:3], (refs[3:6], refs[6]), refs[7:]
    n = len(chunks)
    pools, landed, b1, b2, b3, held = (scratch[i * n : (i + 1) * n] for i in range(6))
    count_g, count_x, count_z, sx, sz, owners, plan = scratch[6 * n : 6 * n + 7]
    own_sem, core_send, core_recv, r_send, r_recv, x_send, x_recv = scratch[6 * n + 7 : 6 * n + 14]
    z_send, z_recv, out_sem, n_send, n_recv, small_sem = scratch[6 * n + 14 :]

    gx, gy = lax.axis_index("gx"), lax.axis_index("gy")
    x, y, z, c = lax.div(gy, 4), lax.div(gx, 2), lax.rem(gy, 4), lax.rem(gx, 2)
    other = 1 - c
    xs = [device(mod4(x + d), y, z, c) for d in range(4)]
    zs = [device(x, y, mod4(z + d), c) for d in range(4)]
    zo = [device(x, y, mod4(z + d), other) for d in range(4)]
    gs = [(lax.rem(gx + d, 8), gy) for d in range(8)]
    above, below = device(x, mod4(y + 1), z, c), device(x, mod4(y - 1), z, c)

    barrier = pltpu.get_barrier_semaphore()
    for peer in gs[1:] + xs[1:] + zs[1:] + zo[1:]:
        pl.semaphore_signal(barrier, inc=1, device_id=peer, device_id_type=MESH)
    small = [
        pltpu.make_async_copy(table_ref, plan, small_sem.at[0]),
        pltpu.make_async_copy(new_owner_ref, owners.at[0], small_sem.at[1]),
        pltpu.make_async_copy(counts_ref, count_g.at[gx], small_sem.at[2]),
    ]
    for copy in small:
        copy.start()

    def columns(owner_c, offset, width):
        return pl.ds(pl.multiple_of(owner_c * half + offset, LANES), width)

    sixteen = pl.ds(pl.multiple_of(c * 16, 16), 16)
    own = []
    for k, (s, offset, width) in enumerate(chunks):
        own.append(
            pltpu.make_async_copy(
                states[s].at[:, :, columns(c, offset, width)], pools[k].at[sixteen], own_sem.at[k]
            )
        )
        own[k].start()
    pl.semaphore_wait(barrier, 16)

    started = []

    def remote(src, dst, send, recv, peer):
        copy = pltpu.make_async_remote_copy(
            src_ref=src, dst_ref=dst, send_sem=send, recv_sem=recv, device_id=peer, device_id_type=MESH
        )
        copy.start()
        started.append(copy)
        return copy

    swapped = [
        remote(
            states[s].at[:, :, columns(other, offset, width)],
            pools[k].at[sixteen],
            core_send.at[k],
            core_recv.at[k],
            zo[0],
        )
        for k, (s, offset, width) in enumerate(chunks)
    ]
    for copy in small:
        copy.wait()
    counted = [remote(counts_ref, count_g.at[gx], n_send.at[d], n_recv.at[d], gs[d]) for d in range(1, 8)]

    def tally_x(copies):
        for copy in copies:
            copy.wait_recv()
        count = jnp.sum(count_g[...].astype(jnp.float32), axis=0)
        sx[...] = count
        count_x[pl.ds(x, 1)] = count.reshape(1, 1, LANES)

    def tally_send_x():
        return [remote(sx, count_x.at[x], n_send.at[7 + d], n_recv.at[7 + d], xs[d]) for d in range(1, 4)]

    def tally_z(copies):
        for copy in copies:
            copy.wait_recv()
        count = jnp.sum(count_x[...], axis=0)
        sz[...] = count
        count_z[pl.ds(z, 1)] = count.reshape(1, 1, LANES)

    def tally_send_z():
        return [remote(sz, count_z.at[z], n_send.at[10 + d], n_recv.at[10 + d], zs[d]) for d in range(1, 4)]

    round1, round2, sent_x, sent_z = {}, {}, {}, {}

    def pick(k, entry, arrived):
        here = pools[k][jnp.minimum(entry, 31)]
        return jnp.where(jnp.full(here.shape, entry, jnp.int32) < 32, here, arrived)

    def steps(size, place):
        lax.fori_loop(0, size, place, 0, unroll=size if size % 2 else size // 2)

    def first_round(k):
        own[k].wait()
        swapped[k].wait_recv()

        def place(j, carry):
            for side in range(2):
                b1[k][side, j] = pools[k][plan[side, j]]
            return carry

        steps(l1, place)
        round1[k] = [
            remote(b1[k].at[0], landed[k].at[pl.ds(0, l1)], r_send.at[k, 0], r_recv.at[k, 0], above),
            remote(b1[k].at[1], landed[k].at[pl.ds(l1, l1)], r_send.at[k, 1], r_recv.at[k, 1], below),
        ]

    def second_round(k):
        for copy in round1[k]:
            copy.wait_recv()

        def place(j, carry):
            for side in range(2):
                b2[k][side, j] = pick(k, plan[2 + side, j], landed[k][side * l1 + j])
            return carry

        steps(l2, place)
        base = 2 * l1
        round2[k] = [
            remote(b2[k].at[0], landed[k].at[pl.ds(base, l2)], r_send.at[k, 2], r_recv.at[k, 2], above),
            remote(b2[k].at[1], landed[k].at[pl.ds(base + l2, l2)], r_send.at[k, 3], r_recv.at[k, 3], below),
        ]

    def along_x(k):
        for copy in round2[k]:
            copy.wait_recv()
        for d in ORDER + (0,):
            base = 4 * mod4(x + d)

            def place(j, carry, d=d, base=base):
                to_z, to_c = lax.div(j, 2), lax.rem(j, 2)
                entry = plan[4, base + 16 * to_c + to_z]
                tile = pick(k, entry, landed[k][jnp.maximum(entry - 32, 0)])
                if d == 0:
                    held[k][x, to_z, to_c] = tile
                else:
                    b3[k][d - 1, to_z, to_c] = tile
                return carry

            lax.fori_loop(0, 8, place, 0, unroll=8)
        sent_x[k] = [remote(b3[k].at[d - 1], held[k].at[x], x_send.at[k, d], x_recv.at[k, d], xs[d]) for d in ORDER]

    def along_z(k):
        s, offset, width = chunks[k]
        for copy in sent_x[k]:
            copy.wait_recv()
        landing = outs[s].at[:, z, :, columns(c, offset, width)]
        sent_z[k] = []
        for d in ORDER + (0,):
            to_z = mod4(z + d)
            sent_z[k].append(
                remote(held[k].at[:, to_z, other], landing, z_send.at[k, 4 + d], z_recv.at[k, 4 + d], zo[d])
            )
            if d:
                sent_z[k].append(remote(held[k].at[:, to_z, c], landing, z_send.at[k, d], z_recv.at[k, d], zs[d]))
        local = pltpu.make_async_copy(held[k].at[:, z, c], landing, out_sem.at[k])
        local.start()
        own[k] = local

    for k in range(min(DEPTH, n)):
        first_round(k)
    for i in range(n + 3):
        if i < n:
            second_round(i)
        if i + DEPTH < n:
            first_round(i + DEPTH)
        if 0 <= i - 3 < n:
            along_z(i - 3)
        if 0 <= i - 1 < n:
            along_x(i - 1)
        if i == 0:
            tally_x(counted)
        if i == 1:
            counted = tally_send_x()
        if i == 3:
            tally_z(counted)
        if i == 4:
            counted = tally_send_z()
    for copy in counted:
        copy.wait_recv()
    totals = jnp.sum(count_z[...], axis=0)
    mine = jnp.where(owners[0] == gx * 16 + gy, totals, 0.0)
    slot_count_ref[...] = jnp.broadcast_to(jnp.sum(mine, axis=1, keepdims=True), (1, LANES))
    for k in range(n):
        own[k].wait()
        for copy in sent_z[k]:
            copy.wait_recv()
    for copy in started:
        copy.wait_send()


def adam_kernel(slot_count, master, first, second, grad, new_master, new_first, new_second):
    scaled = grad[0].astype(jnp.float32) / slot_count[0:1, 0:1]
    moved_first = 0.9 * first[0] + 0.1 * scaled
    moved_second = 0.999 * second[0] + 0.001 * scaled * scaled
    step_dir = moved_first / first_correction / (jnp.sqrt(moved_second / second_correction) + 1e-08)
    new_master[0] = master[0] - 0.01 * (step_dir + 0.1 * master[0])
    new_first[0] = moved_first
    new_second[0] = moved_second


def adam_step(master, first, second, grad, slot_count, block_rows=ADAM_ROWS):
    _, rows, ff = grad.shape
    tile = pl.BlockSpec((1, block_rows, ff), lambda i: (0, i, 0))
    state = jax.ShapeDtypeStruct((1, rows, ff), jnp.float32)
    return pl.pallas_call(
        adam_kernel,
        name="adam",
        grid=(rows // block_rows,),
        out_shape=(state, state, state),
        in_specs=[pl.BlockSpec((1, LANES), lambda i: (0, 0)), tile, tile, tile, tile],
        out_specs=(tile, tile, tile),
    )(slot_count, master, first, second, grad)


def body(old_master, old_first, old_second, new_grad, counts, old_owner, new_owner):
    experts = old_owner.shape[0]
    _, rows, ff = old_master.shape
    quarter, half = ff // 4, ff // 2
    row = (1, experts)
    f32, i32 = jnp.float32, jnp.int32
    dma = pltpu.SemaphoreType.DMA
    landed = jax.ShapeDtypeStruct((4, 4, rows, ff), f32)
    vmem, hbm = pl.BlockSpec(memory_space=pltpu.VMEM), pl.BlockSpec(memory_space=pl.ANY)

    def exchange(kernel, name, number, scratch):
        def run(*operands):
            return pl.pallas_call(
                kernel,
                name=name,
                out_shape=(landed, landed, landed, jax.ShapeDtypeStruct(row, f32)),
                in_specs=[hbm] * 7,
                out_specs=(hbm, hbm, hbm, vmem),
                scratch_shapes=scratch,
                compiler_params=pltpu.CompilerParams(
                    collective_id=number, has_side_effects=True, vmem_limit_bytes=60 * 1024 * 1024
                ),
            )(*operands)

        return run

    tallies = [pltpu.VMEM((8, 1, experts), i32), pltpu.VMEM((4, 1, experts), f32), pltpu.VMEM((4, 1, experts), f32)]
    tallies += [pltpu.VMEM(row, f32), pltpu.VMEM(row, f32)]

    chunks = [(s, offset, LANES) for s in range(3) for offset in range(0, quarter, LANES)]
    n = len(chunks)
    spread = exchange(
        functools.partial(exchange_kernel, chunks, quarter),
        "spread",
        len(TIERS),
        [pltpu.VMEM((experts, rows, w), f32) for _, _, w in chunks]
        + [pltpu.VMEM((3, 4, 4, rows, w), f32) for _, _, w in chunks]
        + [pltpu.VMEM((4, 4, 4, rows, w), f32) for _, _, w in chunks]
        + [pltpu.VMEM((4, 4, 4, rows, w), f32) for _, _, w in chunks]
        + tallies
        + [pltpu.VMEM((2, 1, experts), i32), pltpu.VMEM(row, i32), pltpu.SMEM(row, i32)]
        + [dma((n, 4)), dma((n, 4)), dma((n,)), dma((n, 4)), dma((n, 4)), dma((n, 4)), dma((n, 4))]
        + [dma((n, 4)), dma((n, 4)), dma((n, 4)), dma((n, 4)), dma((n,)), dma((14,)), dma((14,)), dma((4,))],
    )

    pieces = []
    for s, widths in enumerate(WIDTHS):
        offset = 0
        for tiles in widths:
            pieces.append((s, offset, tiles * LANES))
            offset += tiles * LANES
    m = len(pieces)
    branches = [
        exchange(
            functools.partial(routed_kernel, pieces, half, l1, l2),
            f"routed_{l1 + l2}",
            number,
            [pltpu.VMEM((32, rows, w), f32) for _, _, w in pieces]
            + [pltpu.VMEM((2 * l1 + 2 * l2, rows, w), f32) for _, _, w in pieces]
            + [pltpu.VMEM((2, l1, rows, w), f32) for _, _, w in pieces]
            + [pltpu.VMEM((2, l2, rows, w), f32) for _, _, w in pieces]
            + [pltpu.VMEM((3, 4, 2, rows, w), f32) for _, _, w in pieces]
            + [pltpu.VMEM((4, 4, 2, rows, w), f32) for _, _, w in pieces]
            + tallies
            + [pltpu.VMEM((1, 1, experts), i32), pltpu.SMEM((8, experts), i32)]
            + [dma((m,)), dma((m,)), dma((m,)), dma((m, 4)), dma((m, 4)), dma((m, 4)), dma((m, 4))]
            + [dma((m, 8)), dma((m, 8)), dma((m,)), dma((14,)), dma((14,)), dma((3,))],
        )
        for number, (l1, l2) in enumerate(TIERS)
    ]

    old, new = old_owner.reshape(row), new_owner.reshape(row)
    table = pl.pallas_call(
        plan_kernel,
        name="plan",
        out_shape=jax.ShapeDtypeStruct((8, experts), i32),
        in_specs=[vmem, vmem],
        out_specs=vmem,
    )(old, new)
    master, first, second, slot_count = lax.switch(
        table[5, 0],
        branches + [spread],
        table,
        counts.reshape(row),
        old,
        new,
        old_master,
        old_first,
        old_second,
    )
    shape = (1, 16 * rows, ff)
    return adam_step(master.reshape(shape), first.reshape(shape), second.reshape(shape), new_grad, slot_count)


def solution(mesh):
    placed = (
        P("gx", "gy", None),
        P("gx", "gy", None),
        P("gx", "gy", None),
        P(("gx", "gy"), None, None),
        P(None, ("gx", "gy")),
        P(),
        P(),
    )
    out = P(("gx", "gy"), None, None)
    return jax.shard_map(body, mesh=mesh, in_specs=placed, out_specs=(out, out, out), check_vma=False)
```

```python
import functools

import jax
import jax.numpy as jnp
from jax import lax
from jax.experimental import pallas as pl
from jax.experimental.pallas import tpu as pltpu
from jax.sharding import PartitionSpec as P

MESH = pl.DeviceIdType.MESH
LANES = 128
ORDER = (1, 3, 2)
Z_LAG = 2
Y_LAG = 4
ADAM_ROWS = 16
DEPTH = 4
X_AFTER = 3
Z_AFTER = 7
TALLY = 2
TIERS = ((8, 8), (9, 8), (9, 9), (10, 10))
WIDTHS = ((1,) * 6,) * 3

first_correction = 1.0 - 0.9**10
second_correction = 1.0 - 0.999**10


def device(x, y, z, c):
    return (y * 2 + c, x * 4 + z)


def mod4(v):
    return lax.rem(v + 4, 4)


def exchange_kernel(
    chunks, quarter, table_ref, counts_ref, old_owner_ref, new_owner_ref, *refs
):
    states, (outs, slot_count_ref), scratch = refs[:3], (refs[3:6], refs[6]), refs[7:]
    n = len(chunks)
    a_bufs, b_bufs, c_bufs, d_bufs = (scratch[i * n : (i + 1) * n] for i in range(4))
    count_g, count_x, count_z, sx, sz, owners, source_row, source_ref = scratch[4 * n : 4 * n + 8]
    sems = scratch[4 * n + 8 :]
    y1_send, y1_recv, own_sem, core_send, core_recv, x_send, x_recv = sems[:7]
    z_send, z_recv, y2_send, y2_recv, out_sem, n_send, n_recv, small_sem = sems[7:]

    gx, gy = lax.axis_index("gx"), lax.axis_index("gy")
    x, y, z, c = lax.div(gy, 4), lax.div(gx, 2), lax.rem(gy, 4), lax.rem(gx, 2)
    other = 1 - c

    xs = [device(mod4(x + d), y, z, c) for d in range(4)]
    ys = [device(x, mod4(y + d), z, c) for d in range(4)]
    zs = [device(x, y, mod4(z + d), c) for d in range(4)]
    gs = [(lax.rem(gx + d, 8), gy) for d in range(8)]

    barrier = pltpu.get_barrier_semaphore()
    for peer in gs[1:] + xs[1:] + zs[1:]:
        pl.semaphore_signal(barrier, inc=1, device_id=peer, device_id_type=MESH)
    pl.semaphore_wait(barrier, 13)

    started = []

    def remote(src, dst, send, recv, peer):
        copy = pltpu.make_async_remote_copy(
            src_ref=src, dst_ref=dst, send_sem=send, recv_sem=recv, device_id=peer, device_id_type=MESH
        )
        copy.start()
        started.append(copy)
        return copy

    def block(owner_y, owner_c):
        return pl.ds(pl.multiple_of((owner_y * 2 + owner_c) * 16, 16), 16)

    def columns(owner_y, offset, width):
        return pl.ds(pl.multiple_of(owner_y * quarter + offset, LANES), width)

    small = [
        pltpu.make_async_copy(old_owner_ref, owners.at[0], small_sem.at[0]),
        pltpu.make_async_copy(new_owner_ref, owners.at[1], small_sem.at[1]),
        pltpu.make_async_copy(counts_ref, count_g.at[gx], small_sem.at[2]),
    ]
    for copy in small:
        copy.start()
    y1, own, cores = [], [], []
    for k, (s, offset, width) in enumerate(chunks):
        y1.append(
            {
                d: remote(
                    states[s].at[:, :, columns(mod4(y + d), offset, width)],
                    a_bufs[k].at[block(y, c)],
                    y1_send.at[k, d],
                    y1_recv.at[k, d],
                    ys[d],
                )
                for d in ORDER
            }
        )
        mine = states[s].at[:, :, columns(y, offset, width)]
        local = pltpu.make_async_copy(mine, a_bufs[k].at[block(y, c)], own_sem.at[k])
        local.start()
        own.append(local)
        cores.append(
            {0: remote(mine, a_bufs[k].at[block(y, c)], core_send.at[k, 0], core_recv.at[k, 0], gs_partner(x, y, z, other))}
        )
        if k == 0:
            tallies = [
                remote(counts_ref, count_g.at[gx], n_send.at[d], n_recv.at[d], gs[d]) for d in range(1, 8)
            ]

    for copy in small:
        copy.wait()
    old_column = jnp.broadcast_to(owners[0], (LANES, LANES)).T
    new_column = jnp.broadcast_to(owners[1], (LANES, LANES)).T
    lanes = lax.broadcasted_iota(jnp.int32, (LANES, LANES), 1)
    source_row[...] = jnp.sum(jnp.where(new_column == lanes, old_column, 0), axis=0, keepdims=True)
    to_scalar = pltpu.make_async_copy(source_row, source_ref, small_sem.at[3])
    to_scalar.start()

    def forward(k):
        for d in ORDER:
            y1[k][d].wait_recv()
            held = a_bufs[k].at[block(mod4(y - d), c)]
            cores[k][d] = remote(held, held, core_send.at[k, d], core_recv.at[k, d], gs_partner(x, y, z, other))

    sent_x, sent_z, sent_y = {}, {}, {}

    def permute(k):
        own[k].wait()
        for d in range(4):
            cores[k][d].wait_recv()
        for d in range(4):
            base = 4 * mod4(x + d) + 16 * c

            def place(j, carry, d=d, base=base):
                to_z, to_y = lax.div(j, 4), lax.rem(j, 4)
                tile = a_bufs[k][source_ref[0, base + 32 * to_y + to_z]]
                if d == 0:
                    c_bufs[k][x, to_z, to_y] = tile
                else:
                    b_bufs[k][d - 1, to_z, to_y] = tile
                return carry

            lax.fori_loop(0, 16, place, 0, unroll=4)
        sent_x[k] = [
            remote(b_bufs[k].at[d - 1], c_bufs[k].at[x], x_send.at[k, d], x_recv.at[k, d], xs[d]) for d in ORDER
        ]

    def along_z(k):
        for copy in sent_x[k]:
            copy.wait_recv()
        sent_z[k] = [
            remote(
                c_bufs[k].at[:, mod4(z + d)], d_bufs[k].at[:, z], z_send.at[k, d], z_recv.at[k, d], zs[d]
            )
            for d in ORDER
        ]
        d_bufs[k][:, pl.ds(z, 1)] = c_bufs[k][:, pl.ds(z, 1)]

    def along_y(k):
        s, offset, width = chunks[k]
        for copy in sent_z[k]:
            copy.wait_recv()
        landing = outs[s].at[:, :, :, columns(y, offset, width)]
        sent_y[k] = [
            remote(d_bufs[k].at[:, :, mod4(y + d)], landing, y2_send.at[k, d], y2_recv.at[k, d], ys[d])
            for d in ORDER
        ]
        local = pltpu.make_async_copy(d_bufs[k].at[:, :, y], landing, out_sem.at[k])
        local.start()
        own[k] = local

    def tally_x():
        for copy in tallies:
            copy.wait_recv()
        count = jnp.sum(count_g[...].astype(jnp.float32), axis=0)
        sx[...] = count
        count_x[pl.ds(x, 1)] = count.reshape(1, 1, LANES)

    def tally_send_x():
        return [
            remote(sx, count_x.at[x], n_send.at[7 + d], n_recv.at[7 + d], xs[d]) for d in range(1, 4)
        ]

    def tally_z(copies):
        for copy in copies:
            copy.wait_recv()
        count = jnp.sum(count_x[...], axis=0)
        sz[...] = count
        count_z[pl.ds(z, 1)] = count.reshape(1, 1, LANES)

    def tally_send_z():
        return [
            remote(sz, count_z.at[z], n_send.at[10 + d], n_recv.at[10 + d], zs[d]) for d in range(1, 4)
        ]

    counted = None
    for i in range(n + Y_LAG):
        if i < n:
            forward(i)
        if 0 <= i - Y_LAG < n:
            along_y(i - Y_LAG)
        if 0 <= i - Z_LAG < n:
            along_z(i - Z_LAG)
        if i == 1:
            counted = tally_send_x()
        if i == 4:
            counted = tally_send_z()
        if i == 0:
            to_scalar.wait()
        if i < n:
            permute(i)
        if i == 0:
            tally_x()
        if i == 3:
            tally_z(counted)
    for copy in counted:
        copy.wait_recv()
    totals = jnp.sum(count_z[...], axis=0)
    mine = jnp.where(owners[1] == gx * 16 + gy, totals, 0.0)
    slot_count_ref[...] = jnp.broadcast_to(jnp.sum(mine, axis=1, keepdims=True), (1, LANES))
    for k in range(n):
        own[k].wait()
        for copy in sent_y[k]:
            copy.wait_recv()
    for copy in started:
        copy.wait_send()


def gs_partner(x, y, z, other):
    return device(x, y, z, other)


def plan_kernel(old_owner_ref, new_owner_ref, counts_ref, table_ref, tally_ref, tier_ref):
    tally_ref[...] = counts_ref[...]
    f32, i32 = jnp.float32, jnp.int32
    square, row = (LANES, LANES), (8, LANES)
    old, new = (jnp.broadcast_to(ref[...], square) for ref in (old_owner_ref, new_owner_ref))
    sub, lane = lax.broadcasted_iota(i32, square, 0), lax.broadcasted_iota(i32, square, 1)

    dest_down = jnp.sum(jnp.where(old == sub, new, 0).astype(f32), axis=1, keepdims=True)
    dest_down = jnp.broadcast_to(dest_down, square)
    dest_across = dest_down.T.astype(i32)
    dest_down = dest_down.astype(i32)
    shift_down = ((dest_down >> 5) - (sub >> 5)) & 3
    shift_across = ((dest_across >> 5) - (lane >> 5)) & 3
    together = (sub >> 5) == (lane >> 5)

    def tally(mask):
        return jnp.broadcast_to(jnp.sum(jnp.where(mask, 1, 0), axis=0, keepdims=True), row)

    rank = tally(together & (shift_down == shift_across) & (sub < lane))
    n1, n2, n3 = (tally(together & (shift_down == d)) for d in (1, 2, 3))

    lane = lane[:8]
    slot, shift, home, own = dest_across[:8], shift_across[:8], lane >> 5, lane & 31

    def before(v):
        return pltpu.roll(v, 32, 1)

    def after(v):
        return pltpu.roll(v, LANES - 32, 1)

    def loads(up):
        down = n2 - up
        return n1 + up + before(up), n3 + down + after(down)

    up = (n2 + (home & 1)) >> 1
    for parity in (0, 1):
        plus, minus = loads(up)
        gap = jnp.maximum(minus, before(minus)) - jnp.maximum(plus, after(plus))
        step = jnp.where(gap < 0, -((-gap) >> 1), gap >> 1)
        up = jnp.where((home & 1) == parity, jnp.clip(up + step, 0, n2), up)
    down = n2 - up
    plus, minus = loads(up)

    def highest(v):
        return jnp.broadcast_to(jnp.max(v.astype(f32), axis=1, keepdims=True), row).astype(i32)

    need, need_far = highest(jnp.maximum(plus, minus)), highest(jnp.maximum(up, down))
    tier = jnp.full(row, len(TIERS), i32)
    first, second = jnp.full(row, TIERS[-1][0], i32), jnp.full(row, TIERS[-1][1], i32)
    for number, (l1, l2) in reversed(list(enumerate(TIERS))):
        fits = (need <= l1 + l2) & (need_far <= min(l1, l2))
        tier = jnp.where(fits, number, tier)
        first, second = jnp.where(fits, l1, first), jnp.where(fits, l2, second)

    here = lax.div(lax.axis_index("gx"), 2)
    mine, from_before, from_after = (
        home == here,
        home == lax.rem(here + 3, 4),
        home == lax.rem(here + 1, 4),
    )
    goes_up = rank < up
    at_up, at_down = up + rank, down + rank
    late_up, late_down = before(up) + at_up - first, after(down) + at_down - first
    one, two, three = shift == 1, shift == 2, shift == 3

    def pick(*cases):
        value = jnp.full(row, -1, i32)
        for mask, case in cases:
            value = jnp.where(mask, case, value)
        return value

    sends = (
        (pick((mine & two & goes_up, rank), (mine & one & (at_up < first), at_up)), own),
        (pick((mine & two & ~goes_up, rank - up), (mine & three & (at_down < first), at_down)), own),
        (
            pick((mine & one & (at_up >= first), late_up), (from_before & two & goes_up, rank)),
            pick((mine, own), (from_before, 32 + rank)),
        ),
        (
            pick((mine & three & (at_down >= first), late_down), (from_after & two & ~goes_up, rank - up)),
            pick((mine, own), (from_after, 32 + first + rank - up)),
        ),
        (
            pick(((slot >> 5) == here, slot & 31)),
            pick(
                (shift == 0, own),
                (one & (at_up < first), 32 + at_up),
                (one & (at_up >= first), 32 + 2 * first + late_up),
                (three & (at_down < first), 32 + first + at_down),
                (three & (at_down >= first), 32 + 2 * first + second + late_down),
                (two & goes_up, 32 + 2 * first + rank),
                (two & ~goes_up, 32 + 2 * first + second + rank - up),
            ),
        ),
    )
    places = lax.broadcasted_iota(i32, (32, LANES), 0)
    lanes = lax.broadcasted_iota(i32, (32, LANES), 1)
    tier_ref[0] = jnp.max(tier.astype(f32)).astype(i32)
    table = jnp.zeros((32, LANES), f32)
    for k, (position, value) in enumerate(sends):
        hit = jnp.broadcast_to(position[:1], (32, LANES)) == places
        entry = jnp.sum(jnp.where(hit, value[:1], 0).astype(f32), axis=1, keepdims=True)
        table = jnp.where(lanes == k, entry, table)
    table = jnp.concatenate([table, jnp.zeros((LANES - 32, LANES), f32)], axis=0)
    table_ref[...] = table.T[:8].astype(i32)


def routed_kernel(chunks, half, l1, l2, table_ref, counts_ref, old_owner_ref, new_owner_ref, *refs):
    states, (outs, slot_count_ref), scratch = refs[:3], (refs[3:6], refs[6]), refs[7:]
    n = len(chunks)
    pools, landed, b1, b2, b3, held = (scratch[i * n : (i + 1) * n] for i in range(6))
    count_g, count_x, count_z, sx, sz, owners, plan = scratch[6 * n : 6 * n + 7]
    meter, own_sem, send, arrive, n_send, n_recv, small_sem = scratch[6 * n + 7 :]

    gx, gy = lax.axis_index("gx"), lax.axis_index("gy")
    x, y, z, c = lax.div(gy, 4), lax.div(gx, 2), lax.rem(gy, 4), lax.rem(gx, 2)
    other = 1 - c
    xs = [device(mod4(x + d), y, z, c) for d in range(4)]
    zs = [device(x, y, mod4(z + d), c) for d in range(4)]
    zo = [device(x, y, mod4(z + d), other) for d in range(4)]
    gs = [(lax.rem(gx + d, 8), gy) for d in range(8)]
    above, below = device(x, mod4(y + 1), z, c), device(x, mod4(y - 1), z, c)

    barrier = pltpu.get_barrier_semaphore()
    for peer in gs[1:] + xs[1:] + zs[1:] + zo[1:]:
        pl.semaphore_signal(barrier, inc=1, device_id=peer, device_id_type=MESH)
    small = [
        pltpu.make_async_copy(table_ref, plan, small_sem.at[0]),
        pltpu.make_async_copy(new_owner_ref, owners.at[0], small_sem.at[1]),
        pltpu.make_async_copy(counts_ref, count_g.at[gx], small_sem.at[2]),
    ]
    for copy in small:
        copy.start()

    def columns(owner_c, offset, width):
        return pl.ds(pl.multiple_of(owner_c * half + offset, LANES), width)

    sixteen = pl.ds(pl.multiple_of(c * 16, 16), 16)
    own = []
    for k, (s, offset, width) in enumerate(chunks):
        own.append(
            pltpu.make_async_copy(
                states[s].at[:, :, columns(c, offset, width)], pools[k].at[sixteen], own_sem.at[k]
            )
        )
        own[k].start()
    pl.semaphore_wait(barrier, 16)

    def remote(src, dst, sent, landing, peer):
        pltpu.make_async_remote_copy(
            src_ref=src, dst_ref=dst, send_sem=sent, recv_sem=landing, device_id=peer, device_id_type=MESH
        ).start()

    def settle(sem, ref):
        pltpu.make_async_copy(ref, ref, sem).wait()

    for k, (s, offset, width) in enumerate(chunks):
        remote(
            states[s].at[:, :, columns(other, offset, width)], pools[k].at[sixteen], send.at[k], arrive.at[k, 0], zo[0]
        )
    for copy in small:
        copy.wait()
    for peer in gs[1:]:
        remote(counts_ref, count_g.at[gx], n_send.at[0], n_recv.at[0], peer)

    def tally_x():
        settle(n_recv.at[0], count_g.at[pl.ds(0, 7)])
        count = jnp.sum(count_g[...].astype(jnp.float32), axis=0)
        sx[...] = count
        count_x[pl.ds(x, 1)] = count.reshape(1, 1, LANES)

    def tally_send_x():
        for peer in xs[1:]:
            remote(sx, count_x.at[x], n_send.at[1], n_recv.at[1], peer)

    def tally_z():
        settle(n_recv.at[1], count_x.at[pl.ds(0, 3)])
        count = jnp.sum(count_x[...], axis=0)
        sz[...] = count
        count_z[pl.ds(z, 1)] = count.reshape(1, 1, LANES)

    def tally_send_z():
        for peer in zs[1:]:
            remote(sz, count_z.at[z], n_send.at[2], n_recv.at[2], peer)

    def pick(k, entry, arrived):
        here = pools[k][jnp.minimum(entry, 31)]
        return jnp.where(jnp.full(here.shape, entry, jnp.int32) < 32, here, arrived)

    def steps(size, place):
        lax.fori_loop(0, size, place, 0, unroll=size if size % 2 else size // 2)

    def first_round(k):
        own[k].wait()
        settle(arrive.at[k, 0], pools[k].at[pl.ds(0, 16)])

        def place(j, carry):
            for side in range(2):
                b1[k][side, j] = pools[k][plan[side, j]]
            return carry

        steps(l1, place)
        remote(b1[k].at[0], landed[k].at[pl.ds(0, l1)], send.at[k], arrive.at[k, 1], above)
        remote(b1[k].at[1], landed[k].at[pl.ds(l1, l1)], send.at[k], arrive.at[k, 1], below)

    def second_round(k):
        settle(arrive.at[k, 1], landed[k].at[pl.ds(0, 2 * l1)])

        def place(j, carry):
            for side in range(2):
                b2[k][side, j] = pick(k, plan[2 + side, j], landed[k][side * l1 + j])
            return carry

        steps(l2, place)
        base = 2 * l1
        remote(b2[k].at[0], landed[k].at[pl.ds(base, l2)], send.at[k], arrive.at[k, 2], above)
        remote(b2[k].at[1], landed[k].at[pl.ds(base + l2, l2)], send.at[k], arrive.at[k, 2], below)

    def along_x(k):
        settle(arrive.at[k, 2], landed[k].at[pl.ds(2 * l1, 2 * l2)])
        for d in ORDER + (0,):
            base = 4 * mod4(x + d)

            def place(j, carry, d=d, base=base):
                to_z, to_c = lax.div(j, 2), lax.rem(j, 2)
                entry = plan[4, base + 16 * to_c + to_z]
                tile = pick(k, entry, landed[k][jnp.maximum(entry - 32, 0)])
                if d == 0:
                    held[k][x, to_z, to_c] = tile
                else:
                    b3[k][d - 1, to_z, to_c] = tile
                return carry

            lax.fori_loop(0, 8, place, 0, unroll=8)
        for d in ORDER:
            remote(b3[k].at[d - 1], held[k].at[x], send.at[k], arrive.at[k, 3], xs[d])

    def along_z(k):
        s, offset, width = chunks[k]
        settle(arrive.at[k, 3], held[k].at[pl.ds(0, 3)])
        landing = outs[s].at[:, z, :, columns(c, offset, width)]
        for d in ORDER + (0,):
            to_z = mod4(z + d)
            remote(held[k].at[:, to_z, other], landing, send.at[k], arrive.at[k, 4], zo[d])
            if d:
                remote(held[k].at[:, to_z, c], landing, send.at[k], arrive.at[k, 4], zs[d])
        local = pltpu.make_async_copy(held[k].at[:, z, c], landing, own_sem.at[k])
        local.start()
        own[k] = local

    for k in range(min(DEPTH, n)):
        first_round(k)
    for i in range(n + Z_AFTER):
        if i < n:
            second_round(i)
        if i + DEPTH < n:
            first_round(i + DEPTH)
        if 0 <= i - Z_AFTER < n:
            along_z(i - Z_AFTER)
        if 0 <= i - X_AFTER < n:
            along_x(i - X_AFTER)
        if i == TALLY:
            tally_x()
        if i == TALLY + 1:
            tally_send_x()
        if i == TALLY + 3:
            tally_z()
        if i == TALLY + 4:
            tally_send_z()
    settle(n_recv.at[2], count_z.at[pl.ds(0, 3)])
    totals = jnp.sum(count_z[...], axis=0)
    mine = jnp.where(owners[0] == gx * 16 + gy, totals, 0.0)
    slot_count_ref[...] = jnp.broadcast_to(jnp.sum(mine, axis=1, keepdims=True), (1, LANES))
    for k, (_, _, width) in enumerate(chunks):
        own[k].wait()
        settle(arrive.at[k, 4], pools[k].at[pl.ds(0, 28)])
        settle(send.at[k], meter.at[:, :, pl.ds(0, width)])
    settle(n_send.at[0], count_g.at[pl.ds(0, 7)])
    settle(n_send.at[1], count_x.at[pl.ds(0, 3)])
    settle(n_send.at[2], count_z.at[pl.ds(0, 3)])


def adam_kernel(block, slot_count, master, first, second, grad_ref, *refs):
    outs, (grad, moved, in_sem, out_sem) = refs[:3], refs[3:]
    blocks = range(grad.shape[1] // block)
    loads, stores = [], []
    for i in blocks:
        rows = pl.ds(i * block, block)
        loads.append(pltpu.make_async_copy(grad_ref.at[:, rows], grad.at[:, rows], in_sem.at[i]))
        loads[i].start()
    inverse = 1.0 / slot_count[0:1, 0:1]
    for i in blocks:
        rows = pl.ds(i * block, block)
        loads[i].wait()
        scaled = grad[0, rows].astype(jnp.float32) * inverse
        moved_first = 0.9 * first[0, rows] + 0.1 * scaled
        moved_second = 0.999 * second[0, rows] + 0.001 * scaled * scaled
        scale = jnp.sqrt(moved_second * (1.0 / second_correction)) + 1e-08
        step_dir = moved_first * (1.0 / first_correction) / scale
        moved[1, rows] = moved_first
        moved[2, rows] = moved_second
        moved[0, rows] = master[0, rows] - 0.01 * (step_dir + 0.1 * master[0, rows])
        for j in (1, 2, 0):
            stores.append(pltpu.make_async_copy(moved.at[j, rows], outs[j].at[0, rows], out_sem.at[i, j]))
            stores[-1].start()
    for copy in stores:
        copy.wait()


def adam_step(master, first, second, grad, slot_count):
    _, rows, ff = grad.shape
    state = jax.ShapeDtypeStruct((1, rows, ff), jnp.float32)
    vmem, hbm = pl.BlockSpec(memory_space=pltpu.VMEM), pl.BlockSpec(memory_space=pl.ANY)
    blocks = rows // ADAM_ROWS
    return pl.pallas_call(
        functools.partial(adam_kernel, ADAM_ROWS),
        name="adam",
        out_shape=(state, state, state),
        in_specs=[vmem, vmem, vmem, vmem, hbm],
        out_specs=(hbm, hbm, hbm),
        scratch_shapes=[
            pltpu.VMEM(grad.shape, grad.dtype),
            pltpu.VMEM((3, rows, ff), jnp.float32),
            pltpu.SemaphoreType.DMA((blocks,)),
            pltpu.SemaphoreType.DMA((blocks, 3)),
        ],
    )(slot_count, master, first, second, grad)


def body(old_master, old_first, old_second, new_grad, counts, old_owner, new_owner):
    experts = old_owner.shape[0]
    _, rows, ff = old_master.shape
    quarter, half = ff // 4, ff // 2
    row = (1, experts)
    f32, i32 = jnp.float32, jnp.int32
    dma = pltpu.SemaphoreType.DMA
    landed = jax.ShapeDtypeStruct((4, 4, rows, ff), f32)
    vmem, hbm = pl.BlockSpec(memory_space=pltpu.VMEM), pl.BlockSpec(memory_space=pl.ANY)

    def exchange(kernel, name, number, scratch):
        def run(*operands):
            return pl.pallas_call(
                kernel,
                name=name,
                out_shape=(landed, landed, landed, jax.ShapeDtypeStruct(row, f32)),
                in_specs=[hbm] * 7,
                out_specs=(hbm, hbm, hbm, vmem),
                scratch_shapes=scratch,
                compiler_params=pltpu.CompilerParams(
                    collective_id=number, has_side_effects=True, vmem_limit_bytes=60 * 1024 * 1024
                ),
            )(*operands)

        return run

    tallies = [pltpu.VMEM((8, 1, experts), i32), pltpu.VMEM((4, 1, experts), f32), pltpu.VMEM((4, 1, experts), f32)]
    tallies += [pltpu.VMEM(row, f32), pltpu.VMEM(row, f32)]

    chunks = [(s, offset, LANES) for s in range(3) for offset in range(0, quarter, LANES)]
    n = len(chunks)
    spread = exchange(
        functools.partial(exchange_kernel, chunks, quarter),
        "spread",
        len(TIERS),
        [pltpu.VMEM((experts, rows, w), f32) for _, _, w in chunks]
        + [pltpu.VMEM((3, 4, 4, rows, w), f32) for _, _, w in chunks]
        + [pltpu.VMEM((4, 4, 4, rows, w), f32) for _, _, w in chunks]
        + [pltpu.VMEM((4, 4, 4, rows, w), f32) for _, _, w in chunks]
        + tallies
        + [pltpu.VMEM((2, 1, experts), i32), pltpu.VMEM(row, i32), pltpu.SMEM(row, i32)]
        + [dma((n, 4)), dma((n, 4)), dma((n,)), dma((n, 4)), dma((n, 4)), dma((n, 4)), dma((n, 4))]
        + [dma((n, 4)), dma((n, 4)), dma((n, 4)), dma((n, 4)), dma((n,)), dma((14,)), dma((14,)), dma((4,))],
    )

    pieces = []
    for s, widths in enumerate(WIDTHS):
        offset = 0
        for tiles in widths:
            pieces.append((s, offset, tiles * LANES))
            offset += tiles * LANES
    m = len(pieces)
    branches = [
        exchange(
            functools.partial(routed_kernel, pieces, half, l1, l2),
            f"routed_{l1 + l2}",
            number,
            [pltpu.VMEM((32, rows, w), f32) for _, _, w in pieces]
            + [pltpu.VMEM((2 * l1 + 2 * l2, rows, w), f32) for _, _, w in pieces]
            + [pltpu.VMEM((2, l1, rows, w), f32) for _, _, w in pieces]
            + [pltpu.VMEM((2, l2, rows, w), f32) for _, _, w in pieces]
            + [pltpu.VMEM((3, 4, 2, rows, w), f32) for _, _, w in pieces]
            + [pltpu.VMEM((4, 4, 2, rows, w), f32) for _, _, w in pieces]
            + tallies
            + [pltpu.VMEM((1, 1, experts), i32), pltpu.SMEM((8, experts), i32)]
            + [pltpu.VMEM((68 + 2 * l1 + 2 * l2, rows, max(w for _, _, w in pieces)), f32)]
            + [dma((m,)), dma((m,)), dma((m, 5)), dma((3,)), dma((3,)), dma((3,))],
        )
        for number, (l1, l2) in enumerate(TIERS)
    ]

    old, new = old_owner.reshape(row), new_owner.reshape(row)
    table, tally, tier = pl.pallas_call(
        plan_kernel,
        name="plan",
        out_shape=(jax.ShapeDtypeStruct((8, experts), i32), jax.ShapeDtypeStruct(row, i32), jax.ShapeDtypeStruct((1,), i32)),
        in_specs=[vmem, vmem, vmem],
        out_specs=(vmem, vmem, pl.BlockSpec(memory_space=pltpu.SMEM)),
    )(old, new, counts.reshape(row))
    master, first, second, slot_count = lax.switch(
        tier[0],
        branches + [spread],
        table,
        tally,
        old,
        new,
        old_master,
        old_first,
        old_second,
    )
    shape = (1, 16 * rows, ff)
    return adam_step(master.reshape(shape), first.reshape(shape), second.reshape(shape), new_grad, slot_count)


def solution(mesh):
    placed = (
        P("gx", "gy", None),
        P("gx", "gy", None),
        P("gx", "gy", None),
        P(("gx", "gy"), None, None),
        P(None, ("gx", "gy")),
        P(),
        P(),
    )
    out = P(("gx", "gy"), None, None)
    return jax.shard_map(body, mesh=mesh, in_specs=placed, out_specs=(out, out, out), check_vma=False)
```

```python
import functools

import jax
import jax.numpy as jnp
from jax import lax
from jax.experimental import pallas as pl
from jax.experimental.pallas import tpu as pltpu
from jax.sharding import PartitionSpec as P

MESH = pl.DeviceIdType.MESH
LANES = 128
ORDER = (1, 3, 2)
Z_LAG = 2
Y_LAG = 4
ADAM_ROWS = 16
DEPTH = 4
UNROLL = 2
UNROLL_X = 2
X_AFTER = 3
Z_AFTER = 7
TALLY = 2
TIERS = ((8, 8), (9, 8), (9, 9), (10, 10))
WIDTHS = ((1,) * 6,) * 3

first_correction = 1.0 - 0.9**10
second_correction = 1.0 - 0.999**10


def device(x, y, z, c):
    return (y * 2 + c, x * 4 + z)


def mod4(v):
    return lax.rem(v + 4, 4)


def exchange_kernel(
    chunks, quarter, table_ref, counts_ref, owners_ref, *refs
):
    states, (outs, slot_count_ref), scratch = refs[:3], (refs[3:6], refs[6]), refs[7:]
    n = len(chunks)
    a_bufs, b_bufs, c_bufs, d_bufs = (scratch[i * n : (i + 1) * n] for i in range(4))
    count_g, count_x, count_z, sx, sz, owners, source_row, source_ref = scratch[4 * n : 4 * n + 8]
    sems = scratch[4 * n + 8 :]
    y1_send, y1_recv, own_sem, core_send, core_recv, x_send, x_recv = sems[:7]
    z_send, z_recv, y2_send, y2_recv, out_sem, n_send, n_recv, small_sem = sems[7:]

    gx, gy = lax.axis_index("gx"), lax.axis_index("gy")
    x, y, z, c = lax.div(gy, 4), lax.div(gx, 2), lax.rem(gy, 4), lax.rem(gx, 2)
    other = 1 - c

    xs = [device(mod4(x + d), y, z, c) for d in range(4)]
    ys = [device(x, mod4(y + d), z, c) for d in range(4)]
    zs = [device(x, y, mod4(z + d), c) for d in range(4)]
    gs = [(lax.rem(gx + d, 8), gy) for d in range(8)]

    barrier = pltpu.get_barrier_semaphore()
    for peer in gs[1:] + xs[1:] + zs[1:]:
        pl.semaphore_signal(barrier, inc=1, device_id=peer, device_id_type=MESH)
    pl.semaphore_wait(barrier, 13)

    started = []

    def remote(src, dst, send, recv, peer):
        copy = pltpu.make_async_remote_copy(
            src_ref=src, dst_ref=dst, send_sem=send, recv_sem=recv, device_id=peer, device_id_type=MESH
        )
        copy.start()
        started.append(copy)
        return copy

    def block(owner_y, owner_c):
        return pl.ds(pl.multiple_of((owner_y * 2 + owner_c) * 16, 16), 16)

    def columns(owner_y, offset, width):
        return pl.ds(pl.multiple_of(owner_y * quarter + offset, LANES), width)

    small = [
        pltpu.make_async_copy(owners_ref, owners, small_sem.at[0]),
        pltpu.make_async_copy(counts_ref, count_g.at[gx], small_sem.at[2]),
    ]
    for copy in small:
        copy.start()
    y1, own, cores = [], [], []
    for k, (s, offset, width) in enumerate(chunks):
        y1.append(
            {
                d: remote(
                    states[s].at[:, :, columns(mod4(y + d), offset, width)],
                    a_bufs[k].at[block(y, c)],
                    y1_send.at[k, d],
                    y1_recv.at[k, d],
                    ys[d],
                )
                for d in ORDER
            }
        )
        mine = states[s].at[:, :, columns(y, offset, width)]
        local = pltpu.make_async_copy(mine, a_bufs[k].at[block(y, c)], own_sem.at[k])
        local.start()
        own.append(local)
        cores.append(
            {0: remote(mine, a_bufs[k].at[block(y, c)], core_send.at[k, 0], core_recv.at[k, 0], gs_partner(x, y, z, other))}
        )
        if k == 0:
            tallies = [
                remote(counts_ref, count_g.at[gx], n_send.at[d], n_recv.at[d], gs[d]) for d in range(1, 8)
            ]

    for copy in small:
        copy.wait()
    old_column = jnp.broadcast_to(owners[0], (LANES, LANES)).T
    new_column = jnp.broadcast_to(owners[1], (LANES, LANES)).T
    lanes = lax.broadcasted_iota(jnp.int32, (LANES, LANES), 1)
    source_row[...] = jnp.sum(jnp.where(new_column == lanes, old_column, 0), axis=0, keepdims=True)
    to_scalar = pltpu.make_async_copy(source_row, source_ref, small_sem.at[3])
    to_scalar.start()

    def forward(k):
        for d in ORDER:
            y1[k][d].wait_recv()
            held = a_bufs[k].at[block(mod4(y - d), c)]
            cores[k][d] = remote(held, held, core_send.at[k, d], core_recv.at[k, d], gs_partner(x, y, z, other))

    sent_x, sent_z, sent_y = {}, {}, {}

    def permute(k):
        own[k].wait()
        for d in range(4):
            cores[k][d].wait_recv()
        for d in range(4):
            base = 4 * mod4(x + d) + 16 * c

            def place(j, carry, d=d, base=base):
                to_z, to_y = lax.div(j, 4), lax.rem(j, 4)
                tile = a_bufs[k][source_ref[0, base + 32 * to_y + to_z]]
                if d == 0:
                    c_bufs[k][x, to_z, to_y] = tile
                else:
                    b_bufs[k][d - 1, to_z, to_y] = tile
                return carry

            lax.fori_loop(0, 16, place, 0, unroll=4)
        sent_x[k] = [
            remote(b_bufs[k].at[d - 1], c_bufs[k].at[x], x_send.at[k, d], x_recv.at[k, d], xs[d]) for d in ORDER
        ]

    def along_z(k):
        for copy in sent_x[k]:
            copy.wait_recv()
        sent_z[k] = [
            remote(
                c_bufs[k].at[:, mod4(z + d)], d_bufs[k].at[:, z], z_send.at[k, d], z_recv.at[k, d], zs[d]
            )
            for d in ORDER
        ]
        d_bufs[k][:, pl.ds(z, 1)] = c_bufs[k][:, pl.ds(z, 1)]

    def along_y(k):
        s, offset, width = chunks[k]
        for copy in sent_z[k]:
            copy.wait_recv()
        landing = outs[s].at[:, :, :, columns(y, offset, width)]
        sent_y[k] = [
            remote(d_bufs[k].at[:, :, mod4(y + d)], landing, y2_send.at[k, d], y2_recv.at[k, d], ys[d])
            for d in ORDER
        ]
        local = pltpu.make_async_copy(d_bufs[k].at[:, :, y], landing, out_sem.at[k])
        local.start()
        own[k] = local

    def tally_x():
        for copy in tallies:
            copy.wait_recv()
        count = jnp.sum(count_g[...].astype(jnp.float32), axis=0)
        sx[...] = count
        count_x[pl.ds(x, 1)] = count.reshape(1, 1, LANES)

    def tally_send_x():
        return [
            remote(sx, count_x.at[x], n_send.at[7 + d], n_recv.at[7 + d], xs[d]) for d in range(1, 4)
        ]

    def tally_z(copies):
        for copy in copies:
            copy.wait_recv()
        count = jnp.sum(count_x[...], axis=0)
        sz[...] = count
        count_z[pl.ds(z, 1)] = count.reshape(1, 1, LANES)

    def tally_send_z():
        return [
            remote(sz, count_z.at[z], n_send.at[10 + d], n_recv.at[10 + d], zs[d]) for d in range(1, 4)
        ]

    counted = None
    for i in range(n + Y_LAG):
        if i < n:
            forward(i)
        if 0 <= i - Y_LAG < n:
            along_y(i - Y_LAG)
        if 0 <= i - Z_LAG < n:
            along_z(i - Z_LAG)
        if i == 1:
            counted = tally_send_x()
        if i == 4:
            counted = tally_send_z()
        if i == 0:
            to_scalar.wait()
        if i < n:
            permute(i)
        if i == 0:
            tally_x()
        if i == 3:
            tally_z(counted)
    for copy in counted:
        copy.wait_recv()
    totals = jnp.sum(count_z[...], axis=0)
    mine = jnp.where(owners[1] == gx * 16 + gy, totals, 0.0)
    slot_count_ref[...] = jnp.broadcast_to(jnp.sum(mine, axis=1, keepdims=True), (1, LANES))
    for k in range(n):
        own[k].wait()
        for copy in sent_y[k]:
            copy.wait_recv()
    for copy in started:
        copy.wait_send()


def gs_partner(x, y, z, other):
    return device(x, y, z, other)


def plan_kernel(old_owner_ref, new_owner_ref, counts_ref, table_ref, tally_ref, owners, sems):
    loads = [
        pltpu.make_async_copy(old_owner_ref, owners.at[0], sems.at[0]),
        pltpu.make_async_copy(new_owner_ref, owners.at[1], sems.at[1]),
        pltpu.make_async_copy(counts_ref, tally_ref, sems.at[2]),
    ]
    for copy in loads:
        copy.start()
    for copy in loads:
        copy.wait()
    f32, i32 = jnp.float32, jnp.int32
    square, row = (LANES, LANES), (8, LANES)
    old, new = (jnp.broadcast_to(owners[i], square) for i in range(2))
    sub, lane = lax.broadcasted_iota(i32, square, 0), lax.broadcasted_iota(i32, square, 1)

    dest_down = jnp.sum(jnp.where(old == sub, new, 0).astype(f32), axis=1, keepdims=True)
    dest_down = jnp.broadcast_to(dest_down, square)
    dest_across = dest_down.T.astype(i32)
    dest_down = dest_down.astype(i32)
    shift_down = ((dest_down >> 5) - (sub >> 5)) & 3
    shift_across = ((dest_across >> 5) - (lane >> 5)) & 3
    together = (sub >> 5) == (lane >> 5)

    def tally(mask):
        return jnp.broadcast_to(jnp.sum(jnp.where(mask, 1, 0), axis=0, keepdims=True), row)

    rank = tally(together & (shift_down == shift_across) & (sub < lane))
    n1, n2, n3 = (tally(together & (shift_down == d)) for d in (1, 2, 3))

    lane = lane[:8]
    slot, shift, home, own = dest_across[:8], shift_across[:8], lane >> 5, lane & 31

    def before(v):
        return pltpu.roll(v, 32, 1)

    def after(v):
        return pltpu.roll(v, LANES - 32, 1)

    def loads(up):
        down = n2 - up
        return n1 + up + before(up), n3 + down + after(down)

    up = (n2 + (home & 1)) >> 1
    for parity in (0, 1):
        plus, minus = loads(up)
        gap = jnp.maximum(minus, before(minus)) - jnp.maximum(plus, after(plus))
        step = jnp.where(gap < 0, -((-gap) >> 1), gap >> 1)
        up = jnp.where((home & 1) == parity, jnp.clip(up + step, 0, n2), up)
    down = n2 - up
    plus, minus = loads(up)

    def highest(v):
        return jnp.broadcast_to(jnp.max(v.astype(f32), axis=1, keepdims=True), row).astype(i32)

    need, need_far = highest(jnp.maximum(plus, minus)), highest(jnp.maximum(up, down))
    tier = jnp.full(row, len(TIERS), i32)
    first, second = jnp.full(row, TIERS[-1][0], i32), jnp.full(row, TIERS[-1][1], i32)
    for number, (l1, l2) in reversed(list(enumerate(TIERS))):
        fits = (need <= l1 + l2) & (need_far <= min(l1, l2))
        tier = jnp.where(fits, number, tier)
        first, second = jnp.where(fits, l1, first), jnp.where(fits, l2, second)

    here = lax.div(lax.axis_index("gx"), 2)
    mine, from_before, from_after = (
        home == here,
        home == lax.rem(here + 3, 4),
        home == lax.rem(here + 1, 4),
    )
    goes_up = rank < up
    at_up, at_down = up + rank, down + rank
    late_up, late_down = before(up) + at_up - first, after(down) + at_down - first
    one, two, three = shift == 1, shift == 2, shift == 3

    def pick(*cases):
        value = jnp.full(row, -1, i32)
        for mask, case in cases:
            value = jnp.where(mask, case, value)
        return value

    sends = (
        (pick((mine & two & goes_up, rank), (mine & one & (at_up < first), at_up)), own),
        (pick((mine & two & ~goes_up, rank - up), (mine & three & (at_down < first), at_down)), own),
        (
            pick((mine & one & (at_up >= first), late_up), (from_before & two & goes_up, rank)),
            pick((mine, own), (from_before, 32 + rank)),
        ),
        (
            pick((mine & three & (at_down >= first), late_down), (from_after & two & ~goes_up, rank - up)),
            pick((mine, own), (from_after, 32 + first + rank - up)),
        ),
        (
            pick(((slot >> 5) == here, slot & 31)),
            pick(
                (shift == 0, own),
                (one & (at_up < first), 32 + at_up),
                (one & (at_up >= first), 32 + 2 * first + late_up),
                (three & (at_down < first), 32 + first + at_down),
                (three & (at_down >= first), 32 + 2 * first + second + late_down),
                (two & goes_up, 32 + 2 * first + rank),
                (two & ~goes_up, 32 + 2 * first + second + rank - up),
            ),
        ),
    )
    places = lax.broadcasted_iota(i32, (32, LANES), 0)
    lanes = lax.broadcasted_iota(i32, (32, LANES), 1)
    table = jnp.where(lanes == 5, tier[:1], 0).astype(f32)
    for k, (position, value) in enumerate(sends):
        hit = jnp.broadcast_to(position[:1], (32, LANES)) == places
        entry = jnp.sum(jnp.where(hit, value[:1], 0).astype(f32), axis=1, keepdims=True)
        table = jnp.where(lanes == k, entry, table)
    table = jnp.concatenate([table, jnp.zeros((LANES - 32, LANES), f32)], axis=0)
    table_ref[...] = table.T[:8].astype(i32)


def routed_kernel(chunks, half, l1, l2, table_ref, counts_ref, owners_ref, *refs):
    states, (outs, slot_count_ref), scratch = refs[:3], (refs[3:6], refs[6]), refs[7:]
    n = len(chunks)
    pools, landed, b1, b2, b3, held = (scratch[i * n : (i + 1) * n] for i in range(6))
    count_g, count_x, count_z, sx, sz, owners, plan = scratch[6 * n : 6 * n + 7]
    meter, own_sem, send, arrive, n_send, n_recv, small_sem = scratch[6 * n + 7 :]

    gx, gy = lax.axis_index("gx"), lax.axis_index("gy")
    x, y, z, c = lax.div(gy, 4), lax.div(gx, 2), lax.rem(gy, 4), lax.rem(gx, 2)
    other = 1 - c
    xs = [device(mod4(x + d), y, z, c) for d in range(4)]
    zs = [device(x, y, mod4(z + d), c) for d in range(4)]
    zo = [device(x, y, mod4(z + d), other) for d in range(4)]
    gs = [(lax.rem(gx + d, 8), gy) for d in range(8)]
    above, below = device(x, mod4(y + 1), z, c), device(x, mod4(y - 1), z, c)

    barrier = pltpu.get_barrier_semaphore()
    for peer in gs[1:] + xs[1:] + zs[1:] + zo[1:]:
        pl.semaphore_signal(barrier, inc=1, device_id=peer, device_id_type=MESH)
    small = [
        pltpu.make_async_copy(table_ref, plan, small_sem.at[0]),
        pltpu.make_async_copy(owners_ref, owners, small_sem.at[1]),
        pltpu.make_async_copy(counts_ref, count_g.at[gx], small_sem.at[2]),
    ]
    for copy in small:
        copy.start()

    def columns(owner_c, offset, width):
        return pl.ds(pl.multiple_of(owner_c * half + offset, LANES), width)

    sixteen = pl.ds(pl.multiple_of(c * 16, 16), 16)
    own = []
    for k, (s, offset, width) in enumerate(chunks):
        own.append(
            pltpu.make_async_copy(
                states[s].at[:, :, columns(c, offset, width)], pools[k].at[sixteen], own_sem.at[k]
            )
        )
        own[k].start()
    pl.semaphore_wait(barrier, 16)

    def remote(src, dst, sent, landing, peer):
        pltpu.make_async_remote_copy(
            src_ref=src, dst_ref=dst, send_sem=sent, recv_sem=landing, device_id=peer, device_id_type=MESH
        ).start()

    def settle(sem, ref):
        pltpu.make_async_copy(ref, ref, sem).wait()

    for k, (s, offset, width) in enumerate(chunks):
        remote(
            states[s].at[:, :, columns(other, offset, width)], pools[k].at[sixteen], send.at[k], arrive.at[k, 0], zo[0]
        )
    for copy in small:
        copy.wait()

    def tally_x():
        settle(n_recv.at[0], count_g.at[pl.ds(0, 7)])
        count = jnp.sum(count_g[...].astype(jnp.float32), axis=0)
        sx[...] = count
        count_x[pl.ds(x, 1)] = count.reshape(1, 1, LANES)

    def tally_send_x():
        for peer in xs[1:]:
            remote(sx, count_x.at[x], n_send.at[1], n_recv.at[1], peer)

    def tally_z():
        settle(n_recv.at[1], count_x.at[pl.ds(0, 3)])
        count = jnp.sum(count_x[...], axis=0)
        sz[...] = count
        count_z[pl.ds(z, 1)] = count.reshape(1, 1, LANES)

    def tally_send_z():
        for peer in zs[1:]:
            remote(sz, count_z.at[z], n_send.at[2], n_recv.at[2], peer)

    def pick(k, entry, arrived):
        here = pools[k][jnp.minimum(entry, 31)]
        return jnp.where(jnp.full(here.shape, entry, jnp.int32) < 32, here, arrived)

    def steps(size, place):
        lax.fori_loop(0, size, place, 0, unroll=UNROLL)

    def first_round(k):
        own[k].wait()
        settle(arrive.at[k, 0], pools[k].at[pl.ds(0, 16)])

        def place(j, carry):
            for side in range(2):
                b1[k][side, j] = pools[k][plan[side, j]]
            return carry

        steps(l1, place)
        remote(b1[k].at[0], landed[k].at[pl.ds(0, l1)], send.at[k], arrive.at[k, 1], above)
        remote(b1[k].at[1], landed[k].at[pl.ds(l1, l1)], send.at[k], arrive.at[k, 1], below)

    def second_round(k):
        settle(arrive.at[k, 1], landed[k].at[pl.ds(0, 2 * l1)])

        def place(j, carry):
            for side in range(2):
                b2[k][side, j] = pick(k, plan[2 + side, j], landed[k][side * l1 + j])
            return carry

        steps(l2, place)
        base = 2 * l1
        remote(b2[k].at[0], landed[k].at[pl.ds(base, l2)], send.at[k], arrive.at[k, 2], above)
        remote(b2[k].at[1], landed[k].at[pl.ds(base + l2, l2)], send.at[k], arrive.at[k, 2], below)

    def along_x(k):
        settle(arrive.at[k, 2], landed[k].at[pl.ds(2 * l1, 2 * l2)])
        for d in ORDER + (0,):
            base = 4 * mod4(x + d)

            def place(j, carry, d=d, base=base):
                to_z, to_c = lax.div(j, 2), lax.rem(j, 2)
                entry = plan[4, base + 16 * to_c + to_z]
                tile = pick(k, entry, landed[k][jnp.maximum(entry - 32, 0)])
                if d == 0:
                    held[k][x, to_z, to_c] = tile
                else:
                    b3[k][d - 1, to_z, to_c] = tile
                return carry

            lax.fori_loop(0, 8, place, 0, unroll=UNROLL_X)
        for d in ORDER:
            remote(b3[k].at[d - 1], held[k].at[x], send.at[k], arrive.at[k, 3], xs[d])

    def along_z(k):
        s, offset, width = chunks[k]
        settle(arrive.at[k, 3], held[k].at[pl.ds(0, 3)])
        landing = outs[s].at[:, z, :, columns(c, offset, width)]
        for d in ORDER + (0,):
            to_z = mod4(z + d)
            remote(held[k].at[:, to_z, other], landing, send.at[k], arrive.at[k, 4], zo[d])
            if d:
                remote(held[k].at[:, to_z, c], landing, send.at[k], arrive.at[k, 4], zs[d])
        local = pltpu.make_async_copy(held[k].at[:, z, c], landing, own_sem.at[k])
        local.start()
        own[k] = local

    for k in range(min(DEPTH, n)):
        first_round(k)
    for peer in gs[1:]:
        remote(counts_ref, count_g.at[gx], n_send.at[0], n_recv.at[0], peer)
    for i in range(n + Z_AFTER):
        if i < n:
            second_round(i)
        if i + DEPTH < n:
            first_round(i + DEPTH)
        if 0 <= i - Z_AFTER < n:
            along_z(i - Z_AFTER)
        if 0 <= i - X_AFTER < n:
            along_x(i - X_AFTER)
        if i == TALLY:
            tally_x()
        if i == TALLY + 1:
            tally_send_x()
        if i == TALLY + 3:
            tally_z()
        if i == TALLY + 4:
            tally_send_z()
    settle(n_recv.at[2], count_z.at[pl.ds(0, 3)])
    totals = jnp.sum(count_z[...], axis=0)
    mine = jnp.where(owners[1] == gx * 16 + gy, totals, 0.0)
    slot_count_ref[...] = jnp.broadcast_to(jnp.sum(mine, axis=1, keepdims=True), (1, LANES))
    for k, (_, _, width) in enumerate(chunks):
        own[k].wait()
        settle(arrive.at[k, 4], pools[k].at[pl.ds(0, 28)])
        settle(send.at[k], meter.at[:, :, pl.ds(0, width)])
    settle(n_send.at[0], count_g.at[pl.ds(0, 7)])
    settle(n_send.at[1], count_x.at[pl.ds(0, 3)])
    settle(n_send.at[2], count_z.at[pl.ds(0, 3)])


def adam_kernel(block, slot_count, master, first, second, grad_ref, *refs):
    outs, (grad, moved, in_sem, out_sem) = refs[:3], refs[3:]
    blocks = range(grad.shape[1] // block)
    loads, stores = [], []
    for i in blocks:
        rows = pl.ds(i * block, block)
        loads.append(pltpu.make_async_copy(grad_ref.at[:, rows], grad.at[:, rows], in_sem.at[i]))
        loads[i].start()
    inverse = 1.0 / slot_count[0:1, 0:1]
    for i in blocks:
        rows = pl.ds(i * block, block)
        loads[i].wait()
        scaled = grad[0, rows].astype(jnp.float32) * inverse
        moved_first = 0.9 * first[0, rows] + 0.1 * scaled
        moved_second = 0.999 * second[0, rows] + 0.001 * scaled * scaled
        scale = jnp.sqrt(moved_second * (1.0 / second_correction)) + 1e-08
        step_dir = moved_first * (1.0 / first_correction) / scale
        moved[1, rows] = moved_first
        moved[2, rows] = moved_second
        moved[0, rows] = master[0, rows] - 0.01 * (step_dir + 0.1 * master[0, rows])
        for j in (1, 2, 0):
            stores.append(pltpu.make_async_copy(moved.at[j, rows], outs[j].at[0, rows], out_sem.at[i, j]))
            stores[-1].start()
    for copy in stores:
        copy.wait()


def adam_step(master, first, second, grad, slot_count):
    _, rows, ff = grad.shape
    state = jax.ShapeDtypeStruct((1, rows, ff), jnp.float32)
    vmem, hbm = pl.BlockSpec(memory_space=pltpu.VMEM), pl.BlockSpec(memory_space=pl.ANY)
    blocks = rows // ADAM_ROWS
    return pl.pallas_call(
        functools.partial(adam_kernel, ADAM_ROWS),
        name="adam",
        out_shape=(state, state, state),
        in_specs=[vmem, vmem, vmem, vmem, hbm],
        out_specs=(hbm, hbm, hbm),
        scratch_shapes=[
            pltpu.VMEM(grad.shape, grad.dtype),
            pltpu.VMEM((3, rows, ff), jnp.float32),
            pltpu.SemaphoreType.DMA((blocks,)),
            pltpu.SemaphoreType.DMA((blocks, 3)),
        ],
    )(slot_count, master, first, second, grad)


def body(old_master, old_first, old_second, new_grad, counts, old_owner, new_owner):
    experts = old_owner.shape[0]
    _, rows, ff = old_master.shape
    quarter, half = ff // 4, ff // 2
    row = (1, experts)
    f32, i32 = jnp.float32, jnp.int32
    dma = pltpu.SemaphoreType.DMA
    landed = jax.ShapeDtypeStruct((4, 4, rows, ff), f32)
    vmem, hbm = pl.BlockSpec(memory_space=pltpu.VMEM), pl.BlockSpec(memory_space=pl.ANY)

    def exchange(kernel, name, number, scratch):
        def run(*operands):
            return pl.pallas_call(
                kernel,
                name=name,
                out_shape=(landed, landed, landed, jax.ShapeDtypeStruct(row, f32)),
                in_specs=[hbm] * 6,
                out_specs=(hbm, hbm, hbm, vmem),
                scratch_shapes=scratch,
                compiler_params=pltpu.CompilerParams(
                    collective_id=number, has_side_effects=True, vmem_limit_bytes=60 * 1024 * 1024
                ),
            )(*operands)

        return run

    tallies = [pltpu.VMEM((8, 1, experts), i32), pltpu.VMEM((4, 1, experts), f32), pltpu.VMEM((4, 1, experts), f32)]
    tallies += [pltpu.VMEM(row, f32), pltpu.VMEM(row, f32)]

    chunks = [(s, offset, LANES) for s in range(3) for offset in range(0, quarter, LANES)]
    n = len(chunks)
    spread = exchange(
        functools.partial(exchange_kernel, chunks, quarter),
        "spread",
        len(TIERS),
        [pltpu.VMEM((experts, rows, w), f32) for _, _, w in chunks]
        + [pltpu.VMEM((3, 4, 4, rows, w), f32) for _, _, w in chunks]
        + [pltpu.VMEM((4, 4, 4, rows, w), f32) for _, _, w in chunks]
        + [pltpu.VMEM((4, 4, 4, rows, w), f32) for _, _, w in chunks]
        + tallies
        + [pltpu.VMEM((2, 1, experts), i32), pltpu.VMEM(row, i32), pltpu.SMEM(row, i32)]
        + [dma((n, 4)), dma((n, 4)), dma((n,)), dma((n, 4)), dma((n, 4)), dma((n, 4)), dma((n, 4))]
        + [dma((n, 4)), dma((n, 4)), dma((n, 4)), dma((n, 4)), dma((n,)), dma((14,)), dma((14,)), dma((4,))],
    )

    pieces = []
    for s, widths in enumerate(WIDTHS):
        offset = 0
        for tiles in widths:
            pieces.append((s, offset, tiles * LANES))
            offset += tiles * LANES
    m = len(pieces)
    branches = [
        exchange(
            functools.partial(routed_kernel, pieces, half, l1, l2),
            f"routed_{l1 + l2}",
            number,
            [pltpu.VMEM((32, rows, w), f32) for _, _, w in pieces]
            + [pltpu.VMEM((2 * l1 + 2 * l2, rows, w), f32) for _, _, w in pieces]
            + [pltpu.VMEM((2, l1, rows, w), f32) for _, _, w in pieces]
            + [pltpu.VMEM((2, l2, rows, w), f32) for _, _, w in pieces]
            + [pltpu.VMEM((3, 4, 2, rows, w), f32) for _, _, w in pieces]
            + [pltpu.VMEM((4, 4, 2, rows, w), f32) for _, _, w in pieces]
            + tallies
            + [pltpu.VMEM((2, 1, experts), i32), pltpu.SMEM((8, experts), i32)]
            + [pltpu.VMEM((68 + 2 * l1 + 2 * l2, rows, max(w for _, _, w in pieces)), f32)]
            + [dma((m,)), dma((m,)), dma((m, 5)), dma((3,)), dma((3,)), dma((3,))],
        )
        for number, (l1, l2) in enumerate(TIERS)
    ]

    stay = pl.BlockSpec(memory_space=pltpu.HBM)
    table, tally, owners = pl.pallas_call(
        plan_kernel,
        name="plan",
        out_shape=(jax.ShapeDtypeStruct((8, experts), i32), jax.ShapeDtypeStruct(row, i32), jax.ShapeDtypeStruct((2, 1, experts), i32)),
        in_specs=[stay, stay, stay],
        out_specs=(vmem, vmem, vmem),
        scratch_shapes=[dma((3,))],
    )(old_owner.reshape(row), new_owner.reshape(row), counts.reshape(row))
    master, first, second, slot_count = lax.switch(
        table[5, 0],
        branches + [spread],
        table,
        tally,
        owners,
        old_master,
        old_first,
        old_second,
    )
    shape = (1, 16 * rows, ff)
    return adam_step(master.reshape(shape), first.reshape(shape), second.reshape(shape), new_grad, slot_count)


def solution(mesh):
    placed = (
        P("gx", "gy", None),
        P("gx", "gy", None),
        P("gx", "gy", None),
        P(("gx", "gy"), None, None),
        P(None, ("gx", "gy")),
        P(),
        P(),
    )
    out = P(("gx", "gy"), None, None)
    return jax.shard_map(body, mesh=mesh, in_specs=placed, out_specs=(out, out, out), check_vma=False)
```

```python
import functools

import jax
import jax.numpy as jnp
from jax import lax
from jax.experimental import pallas as pl
from jax.experimental.pallas import tpu as pltpu
from jax.sharding import PartitionSpec as P

MESH = pl.DeviceIdType.MESH
LANES = 128
ORDER = (1, 3, 2)
Z_LAG = 2
Y_LAG = 4
ADAM_ROWS = 16
DEPTH = 4
UNROLL = 2
UNROLL_X = 2
X_AFTER = (3, 0, 3)
Z_AFTER = (6.5, 0, 6.5)
TALLY = 2
TIERS = ((8, 8), (9, 8), (9, 9), (10, 9), (10, 10))
WIDTHS = ((1,) * 6,) * 3

first_correction = 1.0 - 0.9**10
second_correction = 1.0 - 0.999**10


def device(x, y, z, c):
    return (y * 2 + c, x * 4 + z)


def mod4(v):
    return lax.rem(v + 4, 4)


def exchange_kernel(
    chunks, quarter, table_ref, counts_ref, owners_ref, *refs
):
    states, (outs, slot_count_ref), scratch = refs[:3], (refs[3:6], refs[6]), refs[7:]
    n = len(chunks)
    a_bufs, b_bufs, c_bufs, d_bufs = (scratch[i * n : (i + 1) * n] for i in range(4))
    count_g, count_x, count_z, sx, sz, owners, source_row, source_ref = scratch[4 * n : 4 * n + 8]
    sems = scratch[4 * n + 8 :]
    y1_send, y1_recv, own_sem, core_send, core_recv, x_send, x_recv = sems[:7]
    z_send, z_recv, y2_send, y2_recv, out_sem, n_send, n_recv, small_sem = sems[7:]

    gx, gy = lax.axis_index("gx"), lax.axis_index("gy")
    x, y, z, c = lax.div(gy, 4), lax.div(gx, 2), lax.rem(gy, 4), lax.rem(gx, 2)
    other = 1 - c

    xs = [device(mod4(x + d), y, z, c) for d in range(4)]
    ys = [device(x, mod4(y + d), z, c) for d in range(4)]
    zs = [device(x, y, mod4(z + d), c) for d in range(4)]
    gs = [(lax.rem(gx + d, 8), gy) for d in range(8)]

    barrier = pltpu.get_barrier_semaphore()
    for peer in gs[1:] + xs[1:] + zs[1:]:
        pl.semaphore_signal(barrier, inc=1, device_id=peer, device_id_type=MESH)
    pl.semaphore_wait(barrier, 13)

    started = []

    def remote(src, dst, send, recv, peer):
        copy = pltpu.make_async_remote_copy(
            src_ref=src, dst_ref=dst, send_sem=send, recv_sem=recv, device_id=peer, device_id_type=MESH
        )
        copy.start()
        started.append(copy)
        return copy

    def block(owner_y, owner_c):
        return pl.ds(pl.multiple_of((owner_y * 2 + owner_c) * 16, 16), 16)

    def columns(owner_y, offset, width):
        return pl.ds(pl.multiple_of(owner_y * quarter + offset, LANES), width)

    small = [
        pltpu.make_async_copy(owners_ref, owners, small_sem.at[0]),
        pltpu.make_async_copy(counts_ref, count_g.at[gx], small_sem.at[2]),
    ]
    for copy in small:
        copy.start()
    y1, own, cores = [], [], []
    for k, (s, offset, width) in enumerate(chunks):
        y1.append(
            {
                d: remote(
                    states[s].at[:, :, columns(mod4(y + d), offset, width)],
                    a_bufs[k].at[block(y, c)],
                    y1_send.at[k, d],
                    y1_recv.at[k, d],
                    ys[d],
                )
                for d in ORDER
            }
        )
        mine = states[s].at[:, :, columns(y, offset, width)]
        local = pltpu.make_async_copy(mine, a_bufs[k].at[block(y, c)], own_sem.at[k])
        local.start()
        own.append(local)
        cores.append(
            {0: remote(mine, a_bufs[k].at[block(y, c)], core_send.at[k, 0], core_recv.at[k, 0], gs_partner(x, y, z, other))}
        )
        if k == 0:
            tallies = [
                remote(counts_ref, count_g.at[gx], n_send.at[d], n_recv.at[d], gs[d]) for d in range(1, 8)
            ]

    for copy in small:
        copy.wait()
    old_column = jnp.broadcast_to(owners[0], (LANES, LANES)).T
    new_column = jnp.broadcast_to(owners[1], (LANES, LANES)).T
    lanes = lax.broadcasted_iota(jnp.int32, (LANES, LANES), 1)
    source_row[...] = jnp.sum(jnp.where(new_column == lanes, old_column, 0), axis=0, keepdims=True)
    to_scalar = pltpu.make_async_copy(source_row, source_ref, small_sem.at[3])
    to_scalar.start()

    def forward(k):
        for d in ORDER:
            y1[k][d].wait_recv()
            held = a_bufs[k].at[block(mod4(y - d), c)]
            cores[k][d] = remote(held, held, core_send.at[k, d], core_recv.at[k, d], gs_partner(x, y, z, other))

    sent_x, sent_z, sent_y = {}, {}, {}

    def permute(k):
        own[k].wait()
        for d in range(4):
            cores[k][d].wait_recv()
        for d in range(4):
            base = 4 * mod4(x + d) + 16 * c

            def place(j, carry, d=d, base=base):
                to_z, to_y = lax.div(j, 4), lax.rem(j, 4)
                tile = a_bufs[k][source_ref[0, base + 32 * to_y + to_z]]
                if d == 0:
                    c_bufs[k][x, to_z, to_y] = tile
                else:
                    b_bufs[k][d - 1, to_z, to_y] = tile
                return carry

            lax.fori_loop(0, 16, place, 0, unroll=4)
        sent_x[k] = [
            remote(b_bufs[k].at[d - 1], c_bufs[k].at[x], x_send.at[k, d], x_recv.at[k, d], xs[d]) for d in ORDER
        ]

    def along_z(k):
        for copy in sent_x[k]:
            copy.wait_recv()
        sent_z[k] = [
            remote(
                c_bufs[k].at[:, mod4(z + d)], d_bufs[k].at[:, z], z_send.at[k, d], z_recv.at[k, d], zs[d]
            )
            for d in ORDER
        ]
        d_bufs[k][:, pl.ds(z, 1)] = c_bufs[k][:, pl.ds(z, 1)]

    def along_y(k):
        s, offset, width = chunks[k]
        for copy in sent_z[k]:
            copy.wait_recv()
        landing = outs[s].at[:, :, :, columns(y, offset, width)]
        sent_y[k] = [
            remote(d_bufs[k].at[:, :, mod4(y + d)], landing, y2_send.at[k, d], y2_recv.at[k, d], ys[d])
            for d in ORDER
        ]
        local = pltpu.make_async_copy(d_bufs[k].at[:, :, y], landing, out_sem.at[k])
        local.start()
        own[k] = local

    def tally_x():
        for copy in tallies:
            copy.wait_recv()
        count = jnp.sum(count_g[...].astype(jnp.float32), axis=0)
        sx[...] = count
        count_x[pl.ds(x, 1)] = count.reshape(1, 1, LANES)

    def tally_send_x():
        return [
            remote(sx, count_x.at[x], n_send.at[7 + d], n_recv.at[7 + d], xs[d]) for d in range(1, 4)
        ]

    def tally_z(copies):
        for copy in copies:
            copy.wait_recv()
        count = jnp.sum(count_x[...], axis=0)
        sz[...] = count
        count_z[pl.ds(z, 1)] = count.reshape(1, 1, LANES)

    def tally_send_z():
        return [
            remote(sz, count_z.at[z], n_send.at[10 + d], n_recv.at[10 + d], zs[d]) for d in range(1, 4)
        ]

    counted = None
    for i in range(n + Y_LAG):
        if i < n:
            forward(i)
        if 0 <= i - Y_LAG < n:
            along_y(i - Y_LAG)
        if 0 <= i - Z_LAG < n:
            along_z(i - Z_LAG)
        if i == 1:
            counted = tally_send_x()
        if i == 4:
            counted = tally_send_z()
        if i == 0:
            to_scalar.wait()
        if i < n:
            permute(i)
        if i == 0:
            tally_x()
        if i == 3:
            tally_z(counted)
    for copy in counted:
        copy.wait_recv()
    totals = jnp.sum(count_z[...], axis=0)
    mine = jnp.where(owners[1] == gx * 16 + gy, totals, 0.0)
    slot_count_ref[...] = jnp.broadcast_to(jnp.sum(mine, axis=1, keepdims=True), (1, LANES))
    for k in range(n):
        own[k].wait()
        for copy in sent_y[k]:
            copy.wait_recv()
    for copy in started:
        copy.wait_send()


def gs_partner(x, y, z, other):
    return device(x, y, z, other)


def plan_kernel(old_owner_ref, new_owner_ref, counts_ref, table_ref, tally_ref, owners, sems):
    loads = [
        pltpu.make_async_copy(old_owner_ref, owners.at[0], sems.at[0]),
        pltpu.make_async_copy(new_owner_ref, owners.at[1], sems.at[1]),
        pltpu.make_async_copy(counts_ref, tally_ref, sems.at[2]),
    ]
    for copy in loads:
        copy.start()
    for copy in loads:
        copy.wait()
    f32, i32 = jnp.float32, jnp.int32
    square, row = (LANES, LANES), (8, LANES)
    old, new = (jnp.broadcast_to(owners[i], square) for i in range(2))
    sub, lane = lax.broadcasted_iota(i32, square, 0), lax.broadcasted_iota(i32, square, 1)

    dest_down = jnp.sum(jnp.where(old == sub, new, 0).astype(f32), axis=1, keepdims=True)
    dest_down = jnp.broadcast_to(dest_down, square)
    dest_across = dest_down.T.astype(i32)
    dest_down = dest_down.astype(i32)
    shift_down = ((dest_down >> 5) - (sub >> 5)) & 3
    shift_across = ((dest_across >> 5) - (lane >> 5)) & 3
    together = (sub >> 5) == (lane >> 5)

    def tally(mask):
        return jnp.broadcast_to(jnp.sum(jnp.where(mask, 1, 0), axis=0, keepdims=True), row)

    rank = tally(together & (shift_down == shift_across) & (sub < lane))
    n1, n2, n3 = (tally(together & (shift_down == d)) for d in (1, 2, 3))

    lane = lane[:8]
    slot, shift, home, own = dest_across[:8], shift_across[:8], lane >> 5, lane & 31

    def before(v):
        return pltpu.roll(v, 32, 1)

    def after(v):
        return pltpu.roll(v, LANES - 32, 1)

    def loads(up):
        down = n2 - up
        return n1 + up + before(up), n3 + down + after(down)

    up = (n2 + (home & 1)) >> 1
    for parity in (0, 1):
        plus, minus = loads(up)
        gap = jnp.maximum(minus, before(minus)) - jnp.maximum(plus, after(plus))
        step = jnp.where(gap < 0, -((-gap) >> 1), gap >> 1)
        up = jnp.where((home & 1) == parity, jnp.clip(up + step, 0, n2), up)
    down = n2 - up
    plus, minus = loads(up)

    def highest(v):
        return jnp.broadcast_to(jnp.max(v.astype(f32), axis=1, keepdims=True), row).astype(i32)

    need, need_far = highest(jnp.maximum(plus, minus)), highest(jnp.maximum(up, down))
    tier = jnp.full(row, len(TIERS), i32)
    first, second = jnp.full(row, TIERS[-1][0], i32), jnp.full(row, TIERS[-1][1], i32)
    for number, (l1, l2) in reversed(list(enumerate(TIERS))):
        fits = (need <= l1 + l2) & (need_far <= min(l1, l2))
        tier = jnp.where(fits, number, tier)
        first, second = jnp.where(fits, l1, first), jnp.where(fits, l2, second)

    here = lax.div(lax.axis_index("gx"), 2)
    mine, from_before, from_after = (
        home == here,
        home == lax.rem(here + 3, 4),
        home == lax.rem(here + 1, 4),
    )
    goes_up = rank < up
    at_up, at_down = up + rank, down + rank
    late_up, late_down = before(up) + at_up - first, after(down) + at_down - first
    one, two, three = shift == 1, shift == 2, shift == 3

    def pick(*cases):
        value = jnp.full(row, -1, i32)
        for mask, case in cases:
            value = jnp.where(mask, case, value)
        return value

    sends = (
        (pick((mine & two & goes_up, rank), (mine & one & (at_up < first), at_up)), own),
        (pick((mine & two & ~goes_up, rank - up), (mine & three & (at_down < first), at_down)), own),
        (
            pick((mine & one & (at_up >= first), late_up), (from_before & two & goes_up, rank)),
            pick((mine, own), (from_before, 32 + rank)),
        ),
        (
            pick((mine & three & (at_down >= first), late_down), (from_after & two & ~goes_up, rank - up)),
            pick((mine, own), (from_after, 32 + first + rank - up)),
        ),
        (
            pick(((slot >> 5) == here, slot & 31)),
            pick(
                (shift == 0, own),
                (one & (at_up < first), 32 + at_up),
                (one & (at_up >= first), 32 + 2 * first + late_up),
                (three & (at_down < first), 32 + first + at_down),
                (three & (at_down >= first), 32 + 2 * first + second + late_down),
                (two & goes_up, 32 + 2 * first + rank),
                (two & ~goes_up, 32 + 2 * first + second + rank - up),
            ),
        ),
    )
    places = lax.broadcasted_iota(i32, (32, LANES), 0)
    lanes = lax.broadcasted_iota(i32, (32, LANES), 1)
    table = jnp.where(lanes == 5, tier[:1], 0).astype(f32)
    for k, (position, value) in enumerate(sends):
        hit = jnp.broadcast_to(position[:1], (32, LANES)) == places
        entry = jnp.sum(jnp.where(hit, value[:1], 0).astype(f32), axis=1, keepdims=True)
        table = jnp.where(lanes == k, entry, table)
    table = jnp.concatenate([table, jnp.zeros((LANES - 32, LANES), f32)], axis=0)
    table_ref[...] = table.T[:8].astype(i32)


def routed_kernel(chunks, half, l1, l2, table_ref, counts_ref, owners_ref, *refs):
    states, (outs, slot_count_ref), scratch = refs[:3], (refs[3:6], refs[6]), refs[7:]
    n = len(chunks)
    pools, landed, b1, b2, b3, held = (scratch[i * n : (i + 1) * n] for i in range(6))
    count_g, count_x, count_z, sx, sz, owners, plan = scratch[6 * n : 6 * n + 7]
    meter, own_sem, send, arrive, n_send, n_recv, small_sem = scratch[6 * n + 7 :]

    gx, gy = lax.axis_index("gx"), lax.axis_index("gy")
    x, y, z, c = lax.div(gy, 4), lax.div(gx, 2), lax.rem(gy, 4), lax.rem(gx, 2)
    other = 1 - c
    xs = [device(mod4(x + d), y, z, c) for d in range(4)]
    zs = [device(x, y, mod4(z + d), c) for d in range(4)]
    zo = [device(x, y, mod4(z + d), other) for d in range(4)]
    gs = [(lax.rem(gx + d, 8), gy) for d in range(8)]
    above, below = device(x, mod4(y + 1), z, c), device(x, mod4(y - 1), z, c)

    barrier = pltpu.get_barrier_semaphore()
    for peer in gs[1:] + xs[1:] + zs[1:] + zo[1:]:
        pl.semaphore_signal(barrier, inc=1, device_id=peer, device_id_type=MESH)
    small = [
        pltpu.make_async_copy(table_ref, plan, small_sem.at[0]),
        pltpu.make_async_copy(owners_ref, owners, small_sem.at[1]),
        pltpu.make_async_copy(counts_ref, count_g.at[gx], small_sem.at[2]),
    ]
    for copy in small:
        copy.start()

    def columns(owner_c, offset, width):
        return pl.ds(pl.multiple_of(owner_c * half + offset, LANES), width)

    sixteen = pl.ds(pl.multiple_of(c * 16, 16), 16)
    own = []
    for k, (s, offset, width) in enumerate(chunks):
        own.append(
            pltpu.make_async_copy(
                states[s].at[:, :, columns(c, offset, width)], pools[k].at[sixteen], own_sem.at[k]
            )
        )
        own[k].start()
    pl.semaphore_wait(barrier, 16)

    def remote(src, dst, sent, landing, peer):
        pltpu.make_async_remote_copy(
            src_ref=src, dst_ref=dst, send_sem=sent, recv_sem=landing, device_id=peer, device_id_type=MESH
        ).start()

    def settle(sem, ref):
        pltpu.make_async_copy(ref, ref, sem).wait()

    for k, (s, offset, width) in enumerate(chunks):
        remote(
            states[s].at[:, :, columns(other, offset, width)], pools[k].at[sixteen], send.at[k], arrive.at[k, 0], zo[0]
        )
    for copy in small:
        copy.wait()

    def tally_x():
        settle(n_recv.at[0], count_g.at[pl.ds(0, 7)])
        count = jnp.sum(count_g[...].astype(jnp.float32), axis=0)
        sx[...] = count
        count_x[pl.ds(x, 1)] = count.reshape(1, 1, LANES)

    def tally_send_x():
        for peer in xs[1:]:
            remote(sx, count_x.at[x], n_send.at[1], n_recv.at[1], peer)

    def tally_z():
        settle(n_recv.at[1], count_x.at[pl.ds(0, 3)])
        count = jnp.sum(count_x[...], axis=0)
        sz[...] = count
        count_z[pl.ds(z, 1)] = count.reshape(1, 1, LANES)

    def tally_send_z():
        for peer in zs[1:]:
            remote(sz, count_z.at[z], n_send.at[2], n_recv.at[2], peer)

    def pick(k, entry, arrived):
        here = pools[k][jnp.minimum(entry, 31)]
        return jnp.where(jnp.full(here.shape, entry, jnp.int32) < 32, here, arrived)

    def steps(size, place):
        lax.fori_loop(0, size, place, 0, unroll=UNROLL)

    def first_round(k):
        own[k].wait()
        settle(arrive.at[k, 0], pools[k].at[pl.ds(0, 16)])

        def place(j, carry):
            for side in range(2):
                b1[k][side, j] = pools[k][plan[side, j]]
            return carry

        steps(l1, place)
        remote(b1[k].at[0], landed[k].at[pl.ds(0, l1)], send.at[k], arrive.at[k, 1], above)
        remote(b1[k].at[1], landed[k].at[pl.ds(l1, l1)], send.at[k], arrive.at[k, 1], below)

    def second_round(k):
        settle(arrive.at[k, 1], landed[k].at[pl.ds(0, 2 * l1)])

        def place(j, carry):
            for side in range(2):
                b2[k][side, j] = pick(k, plan[2 + side, j], landed[k][side * l1 + j])
            return carry

        steps(l2, place)
        base = 2 * l1
        remote(b2[k].at[0], landed[k].at[pl.ds(base, l2)], send.at[k], arrive.at[k, 2], above)
        remote(b2[k].at[1], landed[k].at[pl.ds(base + l2, l2)], send.at[k], arrive.at[k, 2], below)

    def along_x(k):
        settle(arrive.at[k, 2], landed[k].at[pl.ds(2 * l1, 2 * l2)])
        for d in ORDER + (0,):
            base = 4 * mod4(x + d)

            def place(j, carry, d=d, base=base):
                to_z, to_c = lax.div(j, 2), lax.rem(j, 2)
                entry = plan[4, base + 16 * to_c + to_z]
                tile = pick(k, entry, landed[k][jnp.maximum(entry - 32, 0)])
                if d == 0:
                    held[k][x, to_z, to_c] = tile
                else:
                    b3[k][d - 1, to_z, to_c] = tile
                return carry

            lax.fori_loop(0, 8, place, 0, unroll=UNROLL_X)
        for d in ORDER:
            remote(b3[k].at[d - 1], held[k].at[x], send.at[k], arrive.at[k, 3], xs[d])

    def along_z(k):
        s, offset, width = chunks[k]
        settle(arrive.at[k, 3], held[k].at[pl.ds(0, 3)])
        landing = outs[s].at[:, z, :, columns(c, offset, width)]
        for d in ORDER + (0,):
            to_z = mod4(z + d)
            remote(held[k].at[:, to_z, other], landing, send.at[k], arrive.at[k, 4], zo[d])
            if d:
                remote(held[k].at[:, to_z, c], landing, send.at[k], arrive.at[k, 4], zs[d])
        local = pltpu.make_async_copy(held[k].at[:, z, c], landing, own_sem.at[k])
        local.start()
        own[k] = local

    for k in range(min(DEPTH, n)):
        first_round(k)
    for peer in gs[1:]:
        remote(counts_ref, count_g.at[gx], n_send.at[0], n_recv.at[0], peer)
    order = [(k, 0, second_round, k) for k in range(n)]
    order += [(k - DEPTH, 1, first_round, k) for k in range(DEPTH, n)]
    order += [(k + min(Z_AFTER[0] + k * Z_AFTER[1], Z_AFTER[2]), 2, along_z, k) for k in range(n)]
    order += [(k + min(X_AFTER[0] + k * X_AFTER[1], X_AFTER[2]), 3, along_x, k) for k in range(n)]
    steps_of_tally = (tally_x, tally_send_x, tally_z, tally_send_z)
    order += [(TALLY + lag, 4, step, None) for lag, step in zip((0, 1, 3, 4), steps_of_tally)]
    for _, _, stage, k in sorted(order, key=lambda entry: entry[:2]):
        stage() if k is None else stage(k)
    settle(n_recv.at[2], count_z.at[pl.ds(0, 3)])
    totals = jnp.sum(count_z[...], axis=0)
    mine = jnp.where(owners[1] == gx * 16 + gy, totals, 0.0)
    slot_count_ref[...] = jnp.broadcast_to(jnp.sum(mine, axis=1, keepdims=True), (1, LANES))
    for k, (_, _, width) in enumerate(chunks):
        own[k].wait()
        settle(arrive.at[k, 4], pools[k].at[pl.ds(0, 28)])
        settle(send.at[k], meter.at[:, :, pl.ds(0, width)])
    settle(n_send.at[0], count_g.at[pl.ds(0, 7)])
    settle(n_send.at[1], count_x.at[pl.ds(0, 3)])
    settle(n_send.at[2], count_z.at[pl.ds(0, 3)])


def adam_kernel(block, slot_count, master, first, second, grad_ref, *refs):
    outs, (grad, moved, in_sem, out_sem) = refs[:3], refs[3:]
    blocks = range(grad.shape[1] // block)
    loads, stores = [], []
    for i in blocks:
        rows = pl.ds(i * block, block)
        loads.append(pltpu.make_async_copy(grad_ref.at[:, rows], grad.at[:, rows], in_sem.at[i]))
        loads[i].start()
    inverse = 1.0 / slot_count[0:1, 0:1]
    for i in blocks:
        rows = pl.ds(i * block, block)
        loads[i].wait()
        scaled = grad[0, rows].astype(jnp.float32) * inverse
        moved_first = 0.9 * first[0, rows] + 0.1 * scaled
        moved_second = 0.999 * second[0, rows] + 0.001 * scaled * scaled
        scale = jnp.sqrt(moved_second * (1.0 / second_correction)) + 1e-08
        step_dir = moved_first * (1.0 / first_correction) / scale
        moved[1, rows] = moved_first
        moved[2, rows] = moved_second
        moved[0, rows] = master[0, rows] - 0.01 * (step_dir + 0.1 * master[0, rows])
        for j in (1, 2, 0):
            stores.append(pltpu.make_async_copy(moved.at[j, rows], outs[j].at[0, rows], out_sem.at[i, j]))
            stores[-1].start()
    for copy in stores:
        copy.wait()


def adam_step(master, first, second, grad, slot_count):
    _, rows, ff = grad.shape
    state = jax.ShapeDtypeStruct((1, rows, ff), jnp.float32)
    vmem, hbm = pl.BlockSpec(memory_space=pltpu.VMEM), pl.BlockSpec(memory_space=pl.ANY)
    blocks = rows // ADAM_ROWS
    return pl.pallas_call(
        functools.partial(adam_kernel, ADAM_ROWS),
        name="adam",
        out_shape=(state, state, state),
        in_specs=[vmem, vmem, vmem, vmem, hbm],
        out_specs=(hbm, hbm, hbm),
        scratch_shapes=[
            pltpu.VMEM(grad.shape, grad.dtype),
            pltpu.VMEM((3, rows, ff), jnp.float32),
            pltpu.SemaphoreType.DMA((blocks,)),
            pltpu.SemaphoreType.DMA((blocks, 3)),
        ],
    )(slot_count, master, first, second, grad)


def body(old_master, old_first, old_second, new_grad, counts, old_owner, new_owner):
    experts = old_owner.shape[0]
    _, rows, ff = old_master.shape
    quarter, half = ff // 4, ff // 2
    row = (1, experts)
    f32, i32 = jnp.float32, jnp.int32
    dma = pltpu.SemaphoreType.DMA
    landed = jax.ShapeDtypeStruct((4, 4, rows, ff), f32)
    vmem, hbm = pl.BlockSpec(memory_space=pltpu.VMEM), pl.BlockSpec(memory_space=pl.ANY)

    def exchange(kernel, name, number, scratch):
        def run(*operands):
            return pl.pallas_call(
                kernel,
                name=name,
                out_shape=(landed, landed, landed, jax.ShapeDtypeStruct(row, f32)),
                in_specs=[hbm] * 6,
                out_specs=(hbm, hbm, hbm, vmem),
                scratch_shapes=scratch,
                compiler_params=pltpu.CompilerParams(
                    collective_id=number, has_side_effects=True, vmem_limit_bytes=60 * 1024 * 1024
                ),
            )(*operands)

        return run

    tallies = [pltpu.VMEM((8, 1, experts), i32), pltpu.VMEM((4, 1, experts), f32), pltpu.VMEM((4, 1, experts), f32)]
    tallies += [pltpu.VMEM(row, f32), pltpu.VMEM(row, f32)]

    chunks = [(s, offset, LANES) for s in range(3) for offset in range(0, quarter, LANES)]
    n = len(chunks)
    spread = exchange(
        functools.partial(exchange_kernel, chunks, quarter),
        "spread",
        len(TIERS),
        [pltpu.VMEM((experts, rows, w), f32) for _, _, w in chunks]
        + [pltpu.VMEM((3, 4, 4, rows, w), f32) for _, _, w in chunks]
        + [pltpu.VMEM((4, 4, 4, rows, w), f32) for _, _, w in chunks]
        + [pltpu.VMEM((4, 4, 4, rows, w), f32) for _, _, w in chunks]
        + tallies
        + [pltpu.VMEM((2, 1, experts), i32), pltpu.VMEM(row, i32), pltpu.SMEM(row, i32)]
        + [dma((n, 4)), dma((n, 4)), dma((n,)), dma((n, 4)), dma((n, 4)), dma((n, 4)), dma((n, 4))]
        + [dma((n, 4)), dma((n, 4)), dma((n, 4)), dma((n, 4)), dma((n,)), dma((14,)), dma((14,)), dma((4,))],
    )

    pieces = []
    for s, widths in enumerate(WIDTHS):
        offset = 0
        for tiles in widths:
            pieces.append((s, offset, tiles * LANES))
            offset += tiles * LANES
    m = len(pieces)
    branches = [
        exchange(
            functools.partial(routed_kernel, pieces, half, l1, l2),
            f"routed_{l1 + l2}",
            number,
            [pltpu.VMEM((32, rows, w), f32) for _, _, w in pieces]
            + [pltpu.VMEM((2 * l1 + 2 * l2, rows, w), f32) for _, _, w in pieces]
            + [pltpu.VMEM((2, l1, rows, w), f32) for _, _, w in pieces]
            + [pltpu.VMEM((2, l2, rows, w), f32) for _, _, w in pieces]
            + [pltpu.VMEM((3, 4, 2, rows, w), f32) for _, _, w in pieces]
            + [pltpu.VMEM((4, 4, 2, rows, w), f32) for _, _, w in pieces]
            + tallies
            + [pltpu.VMEM((2, 1, experts), i32), pltpu.SMEM((8, experts), i32)]
            + [pltpu.VMEM((68 + 2 * l1 + 2 * l2, rows, max(w for _, _, w in pieces)), f32)]
            + [dma((m,)), dma((m,)), dma((m, 5)), dma((3,)), dma((3,)), dma((3,))],
        )
        for number, (l1, l2) in enumerate(TIERS)
    ]

    stay = pl.BlockSpec(memory_space=pltpu.HBM)
    table, tally, owners = pl.pallas_call(
        plan_kernel,
        name="plan",
        out_shape=(jax.ShapeDtypeStruct((8, experts), i32), jax.ShapeDtypeStruct(row, i32), jax.ShapeDtypeStruct((2, 1, experts), i32)),
        in_specs=[stay, stay, stay],
        out_specs=(vmem, vmem, vmem),
        scratch_shapes=[dma((3,))],
    )(old_owner.reshape(row), new_owner.reshape(row), counts.reshape(row))
    master, first, second, slot_count = lax.switch(
        table[5, 0],
        branches + [spread],
        table,
        tally,
        owners,
        old_master,
        old_first,
        old_second,
    )
    shape = (1, 16 * rows, ff)
    return adam_step(master.reshape(shape), first.reshape(shape), second.reshape(shape), new_grad, slot_count)


def solution(mesh):
    placed = (
        P("gx", "gy", None),
        P("gx", "gy", None),
        P("gx", "gy", None),
        P(("gx", "gy"), None, None),
        P(None, ("gx", "gy")),
        P(),
        P(),
    )
    out = P(("gx", "gy"), None, None)
    return jax.shard_map(body, mesh=mesh, in_specs=placed, out_specs=(out, out, out), check_vma=False)
```
